512 devices in a mesh: slab: 512 (over z, x, y, core).
Axes of the slice: x: 4, y: 8, z: 8, core: 2. Of those that a mesh axis runs over, the one named last changes fastest.
Arguments:
- start_vectors: float32 [2, 512, 256, 256], P(None, 'slab'), may hold values from -6 to 6
- levels: int32 [512, 256, 256], P('slab'), may hold values from 0 to 15
- energies: float32 [16], replicated, may hold values from -4 to 4
Outputs:
- cheb_field: float32 [2, 512, 256, 256], P(None, 'slab')
- lanczos_diag: float32 [2, 8], replicated
- lanczos_off: float32 [2, 7], replicated
- moments: float32 [2, 6], replicated
The draws below stay inside these ranges and needn't reach their ends.
All inputs are finite; a program needn't handle non-finite values.
Results may differ from the reference program's by a relative error of at most 0.0001.
Values sent between devices are 32-bit elements; how exact they have to be, the bound alone decides.
A program may use at most 64 MiB of HBM per device.

```python
import jax
import jax.numpy as jnp
from jax import lax

NY = 256
NX = 256
VECS = 2
LANCZOS = 8
LEVELS = 16
NZ = 512


def place_ends(entries, stream_key, low, largest):
    shape = entries.shape
    index_at = [jax.random.randint(jax.random.fold_in(stream_key, axis), (), 0, shape[axis]) for axis in range(len(shape))]
    entries = entries.at[tuple(index_at)].set(low)
    longest = shape.index(max(shape))
    index_at[longest] = (index_at[longest] + 1) % shape[longest]
    return entries.at[tuple(index_at)].set(largest)


def shard_levels(stream_key, shape, cuts, least, largest):
    loudness = 1.0
    for position, blocks in cuts:
        heights = jax.random.uniform(jax.random.fold_in(jax.random.fold_in(stream_key, 6), position), (blocks,), jnp.float32, least / len(cuts), largest / len(cuts))
        loudness = loudness * jnp.repeat(jnp.exp(heights), shape[position] // blocks).reshape((-1,) + (1,) * (len(shape) - 1 - position))
    return loudness


def normal_values(stream_key, extent, spread, most, shards=(), held_as=jnp.bfloat16):
    array = spread * jax.random.normal(stream_key, extent, jnp.float32)
    if shards:
        array = array * shard_levels(stream_key, extent, shards, -0.22, 0.18)
    return jnp.clip(array, -most, most).astype(held_as)


def setup_inputs(seed: int = 0) -> dict:
    arg_keys = jax.random.split(jax.random.key(seed), 4)
    return {
        "start_vectors": normal_values(arg_keys[0], (VECS, NZ, NY, NX), 1.0, 6.0, ((1, 512),), jnp.float32),
        "levels": place_ends(jax.random.randint(arg_keys[1], (NZ, NY, NX), 0, LEVELS), jax.random.fold_in(arg_keys[1], 1), 0, LEVELS - 1).astype(jnp.int32),
        "energies": jnp.clip(jax.random.uniform(arg_keys[2], (LEVELS,), jnp.float32, -4.0, 4.0), -4.0, 4.0),
    }


def hamiltonian(field, onsite):
    beside = jnp.roll(field, 1, 1) + jnp.roll(field, -1, 1)
    beside = beside + jnp.roll(field, 1, 2) + jnp.roll(field, -1, 2)
    beside = beside + jnp.roll(field, 1, 3) + jnp.roll(field, -1, 3)
    return onsite[None] * field - beside

def inner(first, second):
    return lax.optimization_barrier(jnp.sum(first * second, axis=(1, 2, 3)))

def expand(values):
    return values[:, None, None, None]

def reference(start_vectors, levels, energies):
    onsite = jnp.take(energies, levels, axis=0)
    norm0 = inner(start_vectors, start_vectors)
    vector = start_vectors / expand(jnp.sqrt(norm0))
    previous = jnp.zeros_like(vector)
    beta_prev = jnp.zeros((VECS,), jnp.float32)
    alphas = []
    betas = []
    for step in range(LANCZOS):
        work = hamiltonian(vector, onsite) - expand(beta_prev) * previous
        alpha = inner(vector, work)
        alphas.append(alpha)
        if step < LANCZOS - 1:
            work = work - expand(alpha) * vector
            beta = jnp.sqrt(inner(work, work))
            betas.append(beta)
            previous, vector, beta_prev = (vector, work / expand(beta), beta)
    diag = jnp.stack(alphas, axis=1)
    offd = jnp.stack(betas, axis=1)
    zero_col = jnp.zeros((VECS, 1), jnp.float32)
    left = jnp.concatenate([zero_col, offd], axis=1)
    right = jnp.concatenate([offd, zero_col], axis=1)
    emin = lax.optimization_barrier(jnp.min(diag - left - right, axis=1))
    emax = lax.optimization_barrier(jnp.max(diag + left + right, axis=1))
    center = expand((emax + emin) * 0.5)
    half = expand(0.55 * (emax - emin))

    def scaled(field):
        return (hamiltonian(field, onsite) - center * field) / half
    term0 = start_vectors
    term1 = scaled(term0)
    term2 = 2.0 * scaled(term1) - term0
    term3 = 2.0 * scaled(term2) - term1
    first = inner(term0, term1)
    moments = jnp.stack([first, inner(term0, term2), inner(term0, term3), 2.0 * inner(term2, term2) - norm0, 2.0 * inner(term3, term2) - first, 2.0 * inner(term3, term3) - norm0], axis=1) / norm0[:, None]
    return (term3, diag, offd, moments)
```

```python
import functools

import jax
import jax.numpy as jnp
from jax import lax
from jax.experimental import pallas as pl
from jax.experimental.pallas import tpu as pltpu
from jax.sharding import PartitionSpec as P

STEPS = 8
CHUNKS = 2
BLOCK = 32
MESH = pl.DeviceIdType.MESH


def two_sum(a, b):
    s = a + b
    t = s - a
    return s, (a - (s - t)) + (b - t)


def fast_two_sum(a, b):
    s = a + b
    return s, b - (s - a)


def split(a):
    t = a * 4097.0
    high = t - (t - a)
    return high, a - high


def two_prod(a, b):
    p = a * b
    ah, al = split(a)
    bh, bl = split(b)
    return p, ((ah * bh - p) + ah * bl + al * bh) + al * bl


def pair_add(a, b):
    s, e = two_sum(a[0], b[0])
    return fast_two_sum(s, e + (a[1] + b[1]))


def pair_neg(a):
    return -a[0], -a[1]


def pair_sub(a, b):
    return pair_add(a, pair_neg(b))


def pair_mul(a, b):
    p, e = two_prod(a[0], b[0])
    return fast_two_sum(p, e + (a[0] * b[1] + a[1] * b[0]))


def pair_div(a, b):
    inv = 1.0 / b[0]
    first = a[0] * inv
    p, e = two_prod(first, b[0])
    rest = (a[0] - p) - e + a[1] - first * b[1]
    return fast_two_sum(first, rest * inv)


def tree_rows(rows):
    lost = None
    while len(rows) > 1:
        sums = []
        for a, b in zip(rows[::2], rows[1::2]):
            s, e = two_sum(a, b)
            sums.append(s)
            lost = e if lost is None else lost + e
        rows = sums
    return rows[0], lost


def coefficients(norms, crosses):
    nu = []
    for k in range(STEPS):
        if k == 0:
            nu += [norms[0], crosses[0]]
        elif k < STEPS - 1:
            nu += [pair_sub(norms[k], norms[k - 1]), pair_sub(crosses[k], crosses[k - 1])]
        else:
            twice = pair_add(crosses[k - 1], crosses[k - 1])
            nu += [pair_sub(norms[k], norms[k - 1]), pair_sub(crosses[k], twice)]
    older, old = {}, dict(enumerate(nu))
    ratio = pair_div(old[1], old[0])
    diag, square = [ratio], []
    for k in range(1, STEPS):
        new = {}
        for l in range(k, 2 * STEPS - k):
            term = pair_sub(pair_add(old[l + 1], old[l - 1]), pair_mul(diag[-1], old[l]))
            if k > 1:
                term = pair_sub(term, pair_mul(square[-1], older[l]))
            new[l] = term
        square.append(pair_div(new[k], old[k - 1]))
        next_ratio = pair_div(new[k + 1], new[k])
        diag.append(pair_sub(next_ratio, ratio))
        ratio = next_ratio
        older, old = old, new
    return diag, square


def kernel(
    n,
    group,
    sv_ref,
    lev_ref,
    en_ref,
    field_ref,
    diag_ref,
    off_ref,
    mom_ref,
    basis,
    below,
    above,
    onsite,
    levels,
    gathered,
    row_a,
    row_b,
    near,
    far,
    table,
    load_sem,
    up_send,
    up_recv,
    down_send,
    down_recv,
    near_send,
    near_recv,
    far_send,
    far_recv,
):
    ny, nx = onsite.shape
    rows = ny // CHUNKS
    groups = n // group
    me = lax.axis_index("slab")
    up = lax.rem(me + 1, n)
    down = lax.rem(me + n - 1, n)
    mine = lax.rem(me, group)
    team = me // group

    def near_peer(k):
        place = lax.rem(mine + k, group)
        return place, team * group + place

    def far_peer(k):
        place = lax.rem(team + k, groups)
        return place, place * group + mine

    def load(v, c):
        part = pl.ds(c * rows, rows)
        return pltpu.make_async_copy(
            sv_ref.at[v, 0, part], basis.at[1, v, part], load_sem.at[v * CHUNKS + c]
        )

    load_levels = pltpu.make_async_copy(lev_ref.at[0], levels, load_sem.at[2 * CHUNKS])
    for v in range(2):
        for c in range(CHUNKS):
            load(v, c).start()
    load_levels.start()

    barrier = pltpu.get_barrier_semaphore()

    def greet(device):
        pl.semaphore_signal(barrier, inc=1, device_id=(device,), device_id_type=MESH)

    greet(up)
    greet(down)
    lax.fori_loop(1, group, lambda k, _: greet(near_peer(k)[1]), None)
    lax.fori_loop(1, groups, lambda k, _: greet(far_peer(k)[1]), None)
    pl.semaphore_wait(barrier, group + groups)

    def halo(k, v, c, upward):
        part = pl.ds(c * rows, rows)
        landing, send, recv, device = (
            (below, up_send, up_recv, up) if upward else (above, down_send, down_recv, down)
        )
        return pltpu.make_async_remote_copy(
            src_ref=basis.at[k + 1, v, part],
            dst_ref=landing.at[k, v, part],
            send_sem=send.at[k, v, c],
            recv_sem=recv.at[k, v, c],
            device_id=(device,),
            device_id_type=MESH,
        )

    for v in range(2):
        for c in range(CHUNKS):
            load(v, c).wait()
            halo(0, v, c, True).start()
            halo(0, v, c, False).start()

    energies = [en_ref[i] for i in range(en_ref.shape[0])]
    shift = sum(energies[1:], energies[0]) * (1.0 / len(energies))
    spread = sum((e - shift) * (e - shift) for e in energies) * (1.0 / len(energies))
    width_row = jnp.full((1, nx), spread + 6.0, jnp.float32)
    inv_row = 1.0 / jnp.sqrt(width_row)

    load_levels.wait()

    def place_onsite(b, _):
        part = pl.ds(pl.multiple_of(b * BLOCK, BLOCK), BLOCK)
        ids = levels[part, :]
        value = jnp.full((BLOCK, nx), energies[0], jnp.float32)
        for i in range(1, len(energies)):
            value = jnp.where(ids == i, energies[i], value)
        onsite[part, :] = (value - shift) * inv_row
        for v in range(2):
            basis[0, v, part, :] = jnp.zeros((BLOCK, nx), jnp.float32)
        return None

    lax.fori_loop(0, ny // BLOCK, place_onsite, None)
    gathered[...] = jnp.zeros((8, 128), jnp.float32)

    def fold(x):
        x = (x[0:8] + x[8:16]) + (x[16:24] + x[24:32])
        return x

    def sweep(k, v, c, totals, last):
        def block(b, carry):
            nh, nl, ch, cl = carry
            start = pl.multiple_of(c * rows + b * BLOCK, BLOCK)
            part = pl.ds(start, BLOCK)
            before = pl.ds(pl.multiple_of(lax.rem(start + (ny - 8), ny), 8), 8)
            after = pl.ds(pl.multiple_of(lax.rem(start + BLOCK, ny), 8), 8)
            here = basis[k + 1, v, part, :]
            tall = jnp.concatenate(
                [basis[k + 1, v, before, :], here, basis[k + 1, v, after, :]], axis=0
            )
            height = BLOCK + 16
            beside = pltpu.roll(tall, 1, 0)[8 : 8 + BLOCK]
            beside = beside + pltpu.roll(tall, height - 1, 0)[8 : 8 + BLOCK]
            beside = beside + (pltpu.roll(here, 1, 1) + pltpu.roll(here, nx - 1, 1))
            if last:
                one = (below if c < CHUNKS // 2 else above)[k, v, part, :]
                beside = beside + (one + one)
            else:
                beside = beside + (below[k, v, part, :] + above[k, v, part, :])
            new = onsite[part, :] * here - inv_row * beside
            if not last:
                new = new - basis[k, v, part, :]
                basis[k + 2, v, part, :] = new
            nh, e = two_sum(nh, fold(here * here))
            ch, d = two_sum(ch, fold(new * here))
            return nh, nl + e, ch, cl + d

        return lax.fori_loop(0, rows // BLOCK, block, totals)

    sub = lax.broadcasted_iota(jnp.int32, (8, 128), 0)
    lane = lax.broadcasted_iota(jnp.int32, (8, 128), 1)

    def gather(k, totals):
        high = jnp.zeros((8, 128), jnp.float32)
        low = jnp.zeros((8, 128), jnp.float32)
        for q, (h, l) in enumerate(totals):
            h, e = two_sum(h[:, :128], h[:, 128:])
            l = (l[:, :128] + l[:, 128:]) + e
            for shift_by in (4, 2, 1):
                h, e = two_sum(h, pltpu.roll(h, shift_by, 0))
                l = l + pltpu.roll(l, shift_by, 0) + e
            high = jnp.where(sub == q, h, high)
            low = jnp.where(sub == q, l, low)
        for shift_by in (64, 32, 16, 8, 4, 2, 1):
            high, e = two_sum(high, pltpu.roll(high, shift_by, 1))
            low = low + pltpu.roll(low, shift_by, 1) + e
        target = jnp.where(sub < 4, (sub // 2) * 64 + lax.rem(sub, 2) * 8 + k, 1000)
        gathered[...] += jnp.where(lane == target, high, 0.0) + jnp.where(
            lane == target + 16, low, 0.0
        )

    def step(k, final_sends=False, last=False):
        totals = []
        for v in range(2):
            zero = jnp.zeros((8, nx), jnp.float32)
            total = (zero, zero, zero, zero)
            for c in range(CHUNKS):
                if not last or c < CHUNKS // 2:
                    halo(k, v, c, True).wait_recv()
                if not last or c >= CHUNKS // 2:
                    halo(k, v, c, False).wait_recv()
                total = sweep(k, v, c, total, last)
                if not last:
                    if not final_sends or c < CHUNKS // 2:
                        halo(k + 1, v, c, True).start()
                    if not final_sends or c >= CHUNKS // 2:
                        halo(k + 1, v, c, False).start()
            totals += [total[:2], total[2:]]
        gather(k, totals)

    lax.fori_loop(0, STEPS - 2, lambda k, _: step(k), None)
    step(STEPS - 2, final_sends=True)
    step(STEPS - 1, last=True)

    packed = gathered[...]
    for shift_by in (4, 2, 1):
        packed = packed + pltpu.roll(packed, shift_by, 0)

    row_lane = lax.broadcasted_iota(jnp.int32, (1, 128), 1)
    is_high = lax.rem(row_lane, 64) < 16

    def exchange(row, staging, slots, place, peer, count, send, recv):
        def copy(k, arriving):
            other, device = peer(k)
            slot = other if arriving else place
            return pltpu.make_async_remote_copy(
                src_ref=staging,
                dst_ref=slots.at[slot],
                send_sem=send.at[k],
                recv_sem=recv.at[slot],
                device_id=(device,),
                device_id_type=MESH,
            )

        staging[...] = row
        slots[place] = row
        lax.fori_loop(1, count, lambda k, _: copy(k, False).start(), None)
        lax.fori_loop(1, count, lambda k, _: copy(k, True).wait_recv(), None)
        total, lost = tree_rows([slots[i] for i in range(count)])
        lax.fori_loop(1, count, lambda k, _: copy(k, False).wait_send(), None)
        return jnp.where(is_high, total, total + pltpu.roll(lost, 16, 1))

    row = exchange(packed[0:1], row_a, near, mine, near_peer, group, near_send, near_recv)
    row = exchange(row, row_b, far, team, far_peer, groups, far_send, far_recv)

    tall_row = lax.broadcasted_iota(jnp.int32, (32, 128), 0)
    tall_lane = lax.broadcasted_iota(jnp.int32, (32, 128), 1)
    spread_row = jnp.broadcast_to(row, (32, 128))
    first = jnp.sum(jnp.where(tall_lane == tall_row, spread_row, 0.0), axis=1, keepdims=True)
    second = jnp.sum(
        jnp.where(tall_lane == tall_row + 64, spread_row, 0.0), axis=1, keepdims=True
    )
    table[...] = jnp.where(tall_lane < 64, first, second)

    norms = [(table[k : k + 1, :], table[16 + k : 17 + k, :]) for k in range(STEPS)]
    crosses = [(table[8 + k : 9 + k, :], table[24 + k : 25 + k, :]) for k in range(STEPS)]
    diag, square = coefficients(norms, crosses)

    width = 1.0 / inv_row[:, :128]
    alphas = [shift + width * a[0] for a in diag]
    betas = [width * jnp.sqrt(b[0]) for b in square]
    zero = jnp.zeros((1, 128), jnp.float32)
    left = [zero] + betas
    right = betas + [zero]
    emin = functools.reduce(jnp.minimum, [a - p - q for a, p, q in zip(alphas, left, right)])
    emax = functools.reduce(jnp.maximum, [a + p + q for a, p, q in zip(alphas, left, right)])
    center = (emax + emin) * 0.5
    inv_half = 1.0 / (0.55 * (emax - emin))
    slope = width * inv_half
    offset = (shift - center) * inv_half

    def apply(poly):
        around = [zero] + poly + [zero]
        out = []
        for k in range(len(poly) + 1):
            value = slope * around[k] if k else None
            if k < len(poly):
                value = offset * poly[k] if value is None else value + offset * poly[k]
            if k + 2 < len(around) - 1:
                value = value + slope * around[k + 2]
            out.append(value)
        return out

    t0 = [zero + 1.0]
    t1 = apply(t0)
    t2 = [2.0 * q for q in apply(t1)]
    t2[0] = t2[0] - 1.0
    t3 = [2.0 * q for q in apply(t2)]
    t3 = [q - t1[k] if k < 2 else q for k, q in enumerate(t3)]

    inv_norm = 1.0 / norms[0][0]
    size = [q[0] * inv_norm for q in norms[:4]]
    cross = [q[0] * inv_norm for q in crosses[:3]]
    skip = pair_sub(norms[1], norms[0])[0] * inv_norm
    skip_next = pair_sub(norms[2], norms[0])[0] * inv_norm
    skip_two = pair_sub(crosses[1], crosses[0])[0] * inv_norm
    gram = [
        [zero + 1.0, cross[0], skip, skip_two],
        [cross[0], size[1], cross[1], skip_next],
        [skip, cross[1], size[2], cross[2]],
        [skip_two, skip_next, cross[2], size[3]],
    ]

    def inner(p, q):
        return sum(
            a * sum(b * gram[i][j] for j, b in enumerate(q)) for i, a in enumerate(p)
        )

    d01 = inner(t0, t1)
    moments = [
        d01,
        inner(t0, t2),
        inner(t0, t3),
        2.0 * inner(t2, t2) - 1.0,
        2.0 * inner(t3, t2) - d01,
        2.0 * inner(t3, t3) - 1.0,
    ]

    def emit(ref, values):
        packed = zero
        for k, value in enumerate(values):
            packed = jnp.where(lax.rem(row_lane, 64) == k, value, packed)
        ref[0:1, :] = packed[:, : len(values)]
        ref[1:2, :] = pltpu.roll(packed, 64, 1)[:, : len(values)]

    for v in range(2):
        keep = row_lane < 64 if v == 0 else row_lane >= 64
        scale = [jnp.where(keep, q, pltpu.roll(q, 64, 1)) for q in t3]
        scale = [jnp.concatenate([q, q], axis=1) for q in scale]

        def finish(b, _):
            part = pl.ds(pl.multiple_of(b * BLOCK, BLOCK), BLOCK)
            value = scale[0] * basis[1, v, part, :] + scale[1] * basis[2, v, part, :]
            value = value + scale[2] * basis[3, v, part, :]
            field_ref[v, 0, part, :] = value + scale[3] * basis[4, v, part, :]
            return None

        lax.fori_loop(0, ny // BLOCK, finish, None)

    emit(diag_ref, alphas)
    emit(off_ref, betas)
    emit(mom_ref, moments)

    def drain(k, _):
        for v in range(2):
            for c in range(CHUNKS):
                halo(k, v, c, True).wait_send()
                halo(k, v, c, False).wait_send()
        return None

    lax.fori_loop(0, STEPS - 1, drain, None)
    for v in range(2):
        for c in range(CHUNKS):
            halo(STEPS - 1, v, c, c < CHUNKS // 2).wait_send()


def solution(mesh):
    n = mesh.shape["slab"]
    group = 16 if n >= 128 else 4

    def shards(start_vectors, levels, energies):
        vecs, _, ny, nx = start_vectors.shape
        f32 = jnp.float32
        dma = pltpu.SemaphoreType.DMA
        vmem = pl.BlockSpec(memory_space=pltpu.VMEM)
        hbm = pl.BlockSpec(memory_space=pl.ANY)
        halo_sem = dma((STEPS, vecs, CHUNKS))
        return pl.pallas_call(
            functools.partial(kernel, n, group),
            out_shape=(
                jax.ShapeDtypeStruct(start_vectors.shape, f32),
                jax.ShapeDtypeStruct((vecs, STEPS), f32),
                jax.ShapeDtypeStruct((vecs, STEPS - 1), f32),
                jax.ShapeDtypeStruct((vecs, 6), f32),
            ),
            in_specs=[hbm, hbm, pl.BlockSpec(memory_space=pltpu.SMEM)],
            out_specs=(vmem, vmem, vmem, vmem),
            scratch_shapes=[
                pltpu.VMEM((STEPS + 1, vecs, ny, nx), f32),
                pltpu.VMEM((STEPS, vecs, ny, nx), f32),
                pltpu.VMEM((STEPS, vecs, ny, nx), f32),
                pltpu.VMEM((ny, nx), f32),
                pltpu.VMEM((ny, nx), jnp.int32),
                pltpu.VMEM((8, 128), f32),
                pltpu.VMEM((1, 128), f32),
                pltpu.VMEM((1, 128), f32),
                pltpu.VMEM((group, 1, 128), f32),
                pltpu.VMEM((n // group, 1, 128), f32),
                pltpu.VMEM((32, 128), f32),
                dma((2 * CHUNKS + 1,)),
                halo_sem,
                halo_sem,
                halo_sem,
                halo_sem,
                dma((group,)),
                dma((group,)),
                dma((n // group,)),
                dma((n // group,)),
            ],
            compiler_params=pltpu.CompilerParams(collective_id=0, has_side_effects=True),
        )(start_vectors, levels, energies)

    return jax.shard_map(
        shards,
        mesh=mesh,
        in_specs=(P(None, "slab", None, None), P("slab", None, None), P()),
        out_specs=(P(None, "slab", None, None), P(), P(), P()),
        check_vma=False,
    )
```

```python
import functools

import jax
import jax.numpy as jnp
from jax import lax
from jax.experimental import pallas as pl
from jax.experimental.pallas import tpu as pltpu
from jax.sharding import PartitionSpec as P

STEPS = 8
CHUNKS = 4
BLOCK = 32
MESH = pl.DeviceIdType.MESH


def two_sum(a, b):
    s = a + b
    t = s - a
    return s, (a - (s - t)) + (b - t)


def fast_two_sum(a, b):
    s = a + b
    return s, b - (s - a)


def split(a):
    t = a * 4097.0
    high = t - (t - a)
    return high, a - high


def two_prod(a, b):
    p = a * b
    ah, al = split(a)
    bh, bl = split(b)
    return p, ((ah * bh - p) + ah * bl + al * bh) + al * bl


def pair_add(a, b):
    s, e = two_sum(a[0], b[0])
    return fast_two_sum(s, e + (a[1] + b[1]))


def pair_neg(a):
    return -a[0], -a[1]


def pair_sub(a, b):
    return pair_add(a, pair_neg(b))


def pair_mul(a, b):
    p, e = two_prod(a[0], b[0])
    return fast_two_sum(p, e + (a[0] * b[1] + a[1] * b[0]))


def pair_div(a, b):
    inv = 1.0 / b[0]
    first = a[0] * inv
    p, e = two_prod(first, b[0])
    rest = (a[0] - p) - e + a[1] - first * b[1]
    return fast_two_sum(first, rest * inv)


def tree_rows(rows):
    lost = None
    while len(rows) > 1:
        sums = []
        for a, b in zip(rows[::2], rows[1::2]):
            s, e = two_sum(a, b)
            sums.append(s)
            lost = e if lost is None else lost + e
        rows = sums
    return rows[0], lost


def coefficients(norms, crosses):
    nu = []
    for k in range(STEPS):
        if k == 0:
            nu += [norms[0], crosses[0]]
        elif k < STEPS - 1:
            nu += [pair_sub(norms[k], norms[k - 1]), pair_sub(crosses[k], crosses[k - 1])]
        else:
            twice = pair_add(crosses[k - 1], crosses[k - 1])
            nu += [pair_sub(norms[k], norms[k - 1]), pair_sub(crosses[k], twice)]
    older, old = {}, dict(enumerate(nu))
    ratio = pair_div(old[1], old[0])
    diag, square = [ratio], []
    for k in range(1, STEPS):
        new = {}
        for l in range(k, 2 * STEPS - k):
            term = pair_sub(pair_add(old[l + 1], old[l - 1]), pair_mul(diag[-1], old[l]))
            if k > 1:
                term = pair_sub(term, pair_mul(square[-1], older[l]))
            new[l] = term
        square.append(pair_div(new[k], old[k - 1]))
        next_ratio = pair_div(new[k + 1], new[k])
        diag.append(pair_sub(next_ratio, ratio))
        ratio = next_ratio
        older, old = old, new
    return diag, square


def scaling(en_ref):
    energies = [en_ref[i] for i in range(en_ref.shape[0])]
    shift = sum(energies[1:], energies[0]) * (1.0 / len(energies))
    spread = sum((e - shift) * (e - shift) for e in energies) * (1.0 / len(energies))
    return energies, shift, spread + 6.0


def inverse_width(square, nx):
    return 1.0 / jnp.sqrt(jnp.full((1, nx), square, jnp.float32))


def iterate(
    n,
    group,
    sv_ref,
    lev_ref,
    en_ref,
    row_ref,
    kept_ref,
    basis,
    below,
    above,
    onsite,
    levels,
    gathered,
    row_a,
    row_b,
    near,
    far,
    load_sem,
    keep_sem,
    met,
    up_send,
    up_recv,
    down_send,
    down_recv,
    near_send,
    near_recv,
    far_send,
    far_recv,
):
    ny, nx = onsite.shape
    rows = ny // CHUNKS
    groups = n // group
    me = lax.axis_index("slab")
    up = lax.rem(me + 1, n)
    down = lax.rem(me + n - 1, n)
    mine = lax.rem(me, group)
    team = me // group

    def near_peer(k):
        place = lax.rem(mine + k, group)
        return place, team * group + place

    def far_peer(k):
        place = lax.rem(team + k, groups)
        return place, place * group + mine

    def tell(sem, device):
        pl.semaphore_signal(sem, inc=1, device_id=(device,), device_id_type=MESH)

    barrier = pltpu.get_barrier_semaphore()
    tell(barrier, up)
    tell(barrier, down)

    def load(v, c):
        part = pl.ds(c * rows, rows)
        return pltpu.make_async_copy(
            sv_ref.at[v, 0, part], basis.at[1, v, part], load_sem.at[v * CHUNKS + c]
        )

    load_levels = pltpu.make_async_copy(lev_ref.at[0], levels, load_sem.at[2 * CHUNKS])
    for v in range(2):
        for c in range(CHUNKS):
            load(v, c).start()
    load_levels.start()

    pl.semaphore_wait(barrier, 2)

    rounds = n.bit_length() - 2

    def hear(r):
        pl.semaphore_wait(met.at[r - 1], 2)

    def say(r, distance):
        tell(met.at[r - 1], lax.rem(me + distance, n))
        tell(met.at[r - 1], lax.rem(me + n - distance, n))

    def halo(k, v, c, upward):
        part = pl.ds(c * rows, rows)
        landing, send, recv, device = (
            (below, up_send, up_recv, up) if upward else (above, down_send, down_recv, down)
        )
        return pltpu.make_async_remote_copy(
            src_ref=basis.at[k + 1, v, part],
            dst_ref=landing.at[k, v, part],
            send_sem=send.at[k, v, c],
            recv_sem=recv.at[k, v, c],
            device_id=(device,),
            device_id_type=MESH,
        )

    for v in range(2):
        for c in range(CHUNKS):
            load(v, c).wait()
            halo(0, v, c, True).start()
            halo(0, v, c, False).start()

    energies, shift, square = scaling(en_ref)
    inv_row = inverse_width(square, nx)

    load_levels.wait()

    def place_onsite(b, _):
        part = pl.ds(pl.multiple_of(b * BLOCK, BLOCK), BLOCK)
        ids = levels[part, :]
        value = jnp.full((BLOCK, nx), energies[0], jnp.float32)
        for i in range(1, len(energies)):
            value = jnp.where(ids == i, energies[i], value)
        onsite[part, :] = (value - shift) * inv_row
        for v in range(2):
            basis[0, v, part, :] = jnp.zeros((BLOCK, nx), jnp.float32)
        return None

    lax.fori_loop(0, ny // BLOCK, place_onsite, None)
    gathered[...] = jnp.zeros((8, 128), jnp.float32)

    def fold(x):
        x = (x[0:8] + x[8:16]) + (x[16:24] + x[24:32])
        return x

    def sweep(k, v, c, totals, last):
        def block(b, carry):
            nh, nl, ch, cl = carry
            start = pl.multiple_of(c * rows + b * BLOCK, BLOCK)
            part = pl.ds(start, BLOCK)
            before = pl.ds(pl.multiple_of(lax.rem(start + (ny - 8), ny), 8), 8)
            after = pl.ds(pl.multiple_of(lax.rem(start + BLOCK, ny), 8), 8)
            here = basis[k + 1, v, part, :]
            tall = jnp.concatenate(
                [basis[k + 1, v, before, :], here, basis[k + 1, v, after, :]], axis=0
            )
            height = BLOCK + 16
            beside = pltpu.roll(tall, 1, 0)[8 : 8 + BLOCK]
            beside = beside + pltpu.roll(tall, height - 1, 0)[8 : 8 + BLOCK]
            beside = beside + (pltpu.roll(here, 1, 1) + pltpu.roll(here, nx - 1, 1))
            if last:
                one = (below if c < CHUNKS // 2 else above)[k, v, part, :]
                beside = beside + (one + one)
            else:
                beside = beside + (below[k, v, part, :] + above[k, v, part, :])
            new = onsite[part, :] * here - inv_row * beside
            if not last:
                new = new - basis[k, v, part, :]
                basis[k + 2, v, part, :] = new
            nh, e = two_sum(nh, fold(here * here))
            ch, d = two_sum(ch, fold(new * here))
            return nh, nl + e, ch, cl + d

        return lax.fori_loop(0, rows // BLOCK, block, totals)

    sub = lax.broadcasted_iota(jnp.int32, (8, 128), 0)
    lane = lax.broadcasted_iota(jnp.int32, (8, 128), 1)

    def gather(k, totals):
        high = jnp.zeros((8, 128), jnp.float32)
        low = jnp.zeros((8, 128), jnp.float32)
        for q, (h, l) in enumerate(totals):
            h, e = two_sum(h[:, :128], h[:, 128:])
            l = (l[:, :128] + l[:, 128:]) + e
            for shift_by in (4, 2, 1):
                h, e = two_sum(h, pltpu.roll(h, shift_by, 0))
                l = l + pltpu.roll(l, shift_by, 0) + e
            high = jnp.where(sub == q, h, high)
            low = jnp.where(sub == q, l, low)
        for shift_by in (64, 32, 16, 8, 4, 2, 1):
            high, e = two_sum(high, pltpu.roll(high, shift_by, 1))
            low = low + pltpu.roll(low, shift_by, 1) + e
        target = jnp.where(sub < 4, (sub // 2) * 64 + lax.rem(sub, 2) * 8 + k, 1000)
        gathered[...] += jnp.where(lane == target, high, 0.0) + jnp.where(
            lane == target + 16, low, 0.0
        )

    def step(k, final_sends=False, last=False):
        totals = []
        for v in range(2):
            zero = jnp.zeros((8, nx), jnp.float32)
            total = (zero, zero, zero, zero)
            for c in range(CHUNKS):
                if not last or c < CHUNKS // 2:
                    halo(k, v, c, True).wait_recv()
                if not last or c >= CHUNKS // 2:
                    halo(k, v, c, False).wait_recv()
                total = sweep(k, v, c, total, last)
                if not last:
                    if not final_sends or c < CHUNKS // 2:
                        halo(k + 1, v, c, True).start()
                    if not final_sends or c >= CHUNKS // 2:
                        halo(k + 1, v, c, False).start()
            totals += [total[:2], total[2:]]
        gather(k, totals)

    def keep(k):
        return pltpu.make_async_copy(basis.at[k + 2], kept_ref.at[k], keep_sem.at[k])

    say(1, 1)
    step(0)
    keep(0).start()

    def middle(k, distance):
        @pl.when(k <= rounds)
        def _():
            hear(k)

        @pl.when(k < rounds)
        def _():
            say(k + 1, distance)

        step(k)

        @pl.when(k < 3)
        def _():
            keep(k).start()

        return distance * 2

    lax.fori_loop(1, STEPS - 2, middle, 2)
    for k in (STEPS - 2, STEPS - 1):
        if k <= rounds:
            hear(k)
        if k < rounds:
            say(k + 1, 2**k)
        step(k, final_sends=k == STEPS - 2, last=k == STEPS - 1)
    if rounds == STEPS:
        hear(rounds)

    packed = gathered[...]
    for shift_by in (4, 2, 1):
        packed = packed + pltpu.roll(packed, shift_by, 0)

    row_lane = lax.broadcasted_iota(jnp.int32, (1, 128), 1)
    is_high = lax.rem(row_lane, 64) < 16

    def exchange(row, staging, slots, place, peer, count, send, recv):
        def copy(k, arriving):
            other, device = peer(k)
            slot = other if arriving else place
            return pltpu.make_async_remote_copy(
                src_ref=staging,
                dst_ref=slots.at[slot],
                send_sem=send.at[k],
                recv_sem=recv.at[slot],
                device_id=(device,),
                device_id_type=MESH,
            )

        staging[...] = row
        slots[place] = row
        lax.fori_loop(1, count, lambda k, _: copy(k, False).start(), None)
        lax.fori_loop(1, count, lambda k, _: copy(k, True).wait_recv(), None)
        total, lost = tree_rows([slots[i] for i in range(count)])
        lax.fori_loop(1, count, lambda k, _: copy(k, False).wait_send(), None)
        return jnp.where(is_high, total, total + pltpu.roll(lost, 16, 1))

    row = exchange(packed[0:1], row_a, near, mine, near_peer, group, near_send, near_recv)
    row = exchange(row, row_b, far, team, far_peer, groups, far_send, far_recv)
    row_ref[...] = row

    def drain(k, _):
        for v in range(2):
            for c in range(CHUNKS):
                halo(k, v, c, True).wait_send()
                halo(k, v, c, False).wait_send()
        return None

    lax.fori_loop(0, STEPS - 1, drain, None)
    for v in range(2):
        for c in range(CHUNKS):
            halo(STEPS - 1, v, c, c < CHUNKS // 2).wait_send()
    for k in range(3):
        keep(k).wait()


def combine(
    en_ref,
    row_ref,
    sv_ref,
    kept_ref,
    field_ref,
    diag_ref,
    off_ref,
    mom_ref,
    basis,
    field,
    table,
    load_sem,
    out_sem,
):
    ny, nx = field.shape[1:]

    def load(v, k):
        source = kept_ref.at[k - 1, v] if k else sv_ref.at[v, 0]
        return pltpu.make_async_copy(source, basis.at[k, v], load_sem.at[v, k])

    for v in range(2):
        for k in range(4):
            load(v, k).start()

    _, shift, square = scaling(en_ref)
    inv_row = inverse_width(square, 128)
    row = row_ref[...]
    row_lane = lax.broadcasted_iota(jnp.int32, (1, 128), 1)
    tall_row = lax.broadcasted_iota(jnp.int32, (32, 128), 0)
    tall_lane = lax.broadcasted_iota(jnp.int32, (32, 128), 1)
    spread_row = jnp.broadcast_to(row, (32, 128))
    first = jnp.sum(jnp.where(tall_lane == tall_row, spread_row, 0.0), axis=1, keepdims=True)
    second = jnp.sum(
        jnp.where(tall_lane == tall_row + 64, spread_row, 0.0), axis=1, keepdims=True
    )
    table[...] = jnp.where(tall_lane < 64, first, second)

    norms = [(table[k : k + 1, :], table[16 + k : 17 + k, :]) for k in range(STEPS)]
    crosses = [(table[8 + k : 9 + k, :], table[24 + k : 25 + k, :]) for k in range(STEPS)]
    diag, square = coefficients(norms, crosses)

    width = 1.0 / inv_row
    alphas = [shift + width * a[0] for a in diag]
    betas = [width * jnp.sqrt(b[0]) for b in square]
    zero = jnp.zeros((1, 128), jnp.float32)
    left = [zero] + betas
    right = betas + [zero]
    emin = functools.reduce(jnp.minimum, [a - p - q for a, p, q in zip(alphas, left, right)])
    emax = functools.reduce(jnp.maximum, [a + p + q for a, p, q in zip(alphas, left, right)])
    center = (emax + emin) * 0.5
    inv_half = 1.0 / (0.55 * (emax - emin))
    slope = width * inv_half
    offset = (shift - center) * inv_half

    def apply(poly):
        around = [zero] + poly + [zero]
        out = []
        for k in range(len(poly) + 1):
            value = slope * around[k] if k else None
            if k < len(poly):
                value = offset * poly[k] if value is None else value + offset * poly[k]
            if k + 2 < len(around) - 1:
                value = value + slope * around[k + 2]
            out.append(value)
        return out

    t0 = [zero + 1.0]
    t1 = apply(t0)
    t2 = [2.0 * q for q in apply(t1)]
    t2[0] = t2[0] - 1.0
    t3 = [2.0 * q for q in apply(t2)]
    t3 = [q - t1[k] if k < 2 else q for k, q in enumerate(t3)]

    inv_norm = 1.0 / norms[0][0]
    size = [q[0] * inv_norm for q in norms[:4]]
    cross = [q[0] * inv_norm for q in crosses[:3]]
    skip = pair_sub(norms[1], norms[0])[0] * inv_norm
    skip_next = pair_sub(norms[2], norms[0])[0] * inv_norm
    skip_two = pair_sub(crosses[1], crosses[0])[0] * inv_norm
    gram = [
        [zero + 1.0, cross[0], skip, skip_two],
        [cross[0], size[1], cross[1], skip_next],
        [skip, cross[1], size[2], cross[2]],
        [skip_two, skip_next, cross[2], size[3]],
    ]

    def inner(p, q):
        return sum(
            a * sum(b * gram[i][j] for j, b in enumerate(q)) for i, a in enumerate(p)
        )

    d01 = inner(t0, t1)
    moments = [
        d01,
        inner(t0, t2),
        inner(t0, t3),
        2.0 * inner(t2, t2) - 1.0,
        2.0 * inner(t3, t2) - d01,
        2.0 * inner(t3, t3) - 1.0,
    ]

    def emit(ref, values):
        packed = zero
        for k, value in enumerate(values):
            packed = jnp.where(lax.rem(row_lane, 64) == k, value, packed)
        ref[0:1, :] = packed[:, : len(values)]
        ref[1:2, :] = pltpu.roll(packed, 64, 1)[:, : len(values)]

    def store(v):
        return pltpu.make_async_copy(field.at[v], field_ref.at[v, 0], out_sem.at[v])

    for v in range(2):
        own = row_lane < 64 if v == 0 else row_lane >= 64
        scale = [jnp.where(own, q, pltpu.roll(q, 64, 1)) for q in t3]
        scale = [jnp.concatenate([q, q], axis=1) for q in scale]
        for k in range(4):
            load(v, k).wait()

        def finish(b, _):
            part = pl.ds(pl.multiple_of(b * BLOCK, BLOCK), BLOCK)
            value = scale[0] * basis[0, v, part, :] + scale[1] * basis[1, v, part, :]
            value = value + scale[2] * basis[2, v, part, :]
            field[v, part, :] = value + scale[3] * basis[3, v, part, :]
            return None

        lax.fori_loop(0, ny // BLOCK, finish, None)
        store(v).start()

    emit(diag_ref, alphas)
    emit(off_ref, betas)
    emit(mom_ref, moments)
    for v in range(2):
        store(v).wait()


def solution(mesh):
    n = mesh.shape["slab"]
    group = 16 if n >= 128 else 4

    def shards(start_vectors, levels, energies):
        vecs, _, ny, nx = start_vectors.shape
        f32 = jnp.float32
        dma = pltpu.SemaphoreType.DMA
        vmem = pl.BlockSpec(memory_space=pltpu.VMEM)
        hbm = pl.BlockSpec(memory_space=pl.ANY)
        halo_sem = dma((STEPS, vecs, CHUNKS))
        smem = pl.BlockSpec(memory_space=pltpu.SMEM)
        groups = n // group
        row, kept = pl.pallas_call(
            functools.partial(iterate, n, group),
            out_shape=(
                jax.ShapeDtypeStruct((1, 128), f32),
                jax.ShapeDtypeStruct((3, vecs, ny, nx), f32),
            ),
            in_specs=[hbm, hbm, smem],
            out_specs=(vmem, hbm),
            scratch_shapes=[
                pltpu.VMEM((STEPS + 1, vecs, ny, nx), f32),
                pltpu.VMEM((STEPS, vecs, ny, nx), f32),
                pltpu.VMEM((STEPS, vecs, ny, nx), f32),
                pltpu.VMEM((ny, nx), f32),
                pltpu.VMEM((ny, nx), jnp.int32),
                pltpu.VMEM((8, 128), f32),
                pltpu.VMEM((1, 128), f32),
                pltpu.VMEM((1, 128), f32),
                pltpu.VMEM((group, 1, 128), f32),
                pltpu.VMEM((groups, 1, 128), f32),
                dma((2 * CHUNKS + 1,)),
                dma((3,)),
                pltpu.SemaphoreType.REGULAR((STEPS,)),
                halo_sem,
                halo_sem,
                halo_sem,
                halo_sem,
                dma((group,)),
                dma((group,)),
                dma((groups,)),
                dma((groups,)),
            ],
            compiler_params=pltpu.CompilerParams(collective_id=0, has_side_effects=True),
        )(start_vectors, levels, energies)
        return pl.pallas_call(
            combine,
            out_shape=(
                jax.ShapeDtypeStruct(start_vectors.shape, f32),
                jax.ShapeDtypeStruct((vecs, STEPS), f32),
                jax.ShapeDtypeStruct((vecs, STEPS - 1), f32),
                jax.ShapeDtypeStruct((vecs, 6), f32),
            ),
            in_specs=[smem, vmem, hbm, hbm],
            out_specs=(hbm, vmem, vmem, vmem),
            scratch_shapes=[
                pltpu.VMEM((4, vecs, ny, nx), f32),
                pltpu.VMEM((vecs, ny, nx), f32),
                pltpu.VMEM((32, 128), f32),
                dma((vecs, 4)),
                dma((vecs,)),
            ],
        )(energies, row, start_vectors, kept)

    return jax.shard_map(
        shards,
        mesh=mesh,
        in_specs=(P(None, "slab", None, None), P("slab", None, None), P()),
        out_specs=(P(None, "slab", None, None), P(), P(), P()),
        check_vma=False,
    )
```

```python
import functools

import jax
import jax.numpy as jnp
from jax import lax
from jax.experimental import pallas as pl
from jax.experimental.pallas import tpu as pltpu
from jax.sharding import PartitionSpec as P

STEPS = 8
CHUNKS = 4
BLOCK = 32
MESH = pl.DeviceIdType.MESH


def two_sum(a, b):
    s = a + b
    t = s - a
    return s, (a - (s - t)) + (b - t)


def fast_two_sum(a, b):
    s = a + b
    return s, b - (s - a)


def split(a):
    t = a * 4097.0
    high = t - (t - a)
    return high, a - high


def two_prod(a, b):
    p = a * b
    ah, al = split(a)
    bh, bl = split(b)
    return p, ((ah * bh - p) + ah * bl + al * bh) + al * bl


def pair_add(a, b):
    s, e = two_sum(a[0], b[0])
    return fast_two_sum(s, e + (a[1] + b[1]))


def pair_neg(a):
    return -a[0], -a[1]


def pair_sub(a, b):
    return pair_add(a, pair_neg(b))


def pair_mul(a, b):
    p, e = two_prod(a[0], b[0])
    return fast_two_sum(p, e + (a[0] * b[1] + a[1] * b[0]))


def pair_div(a, b):
    inv = 1.0 / b[0]
    first = a[0] * inv
    p, e = two_prod(first, b[0])
    rest = (a[0] - p) - e + a[1] - first * b[1]
    return fast_two_sum(first, rest * inv)


def tree_rows(rows):
    lost = None
    while len(rows) > 1:
        sums = []
        for a, b in zip(rows[::2], rows[1::2]):
            s, e = two_sum(a, b)
            sums.append(s)
            lost = e if lost is None else lost + e
        rows = sums
    return rows[0], lost


def coefficients(norms, crosses):
    nu = []
    for k in range(STEPS):
        if k == 0:
            nu += [norms[0], crosses[0]]
        elif k < STEPS - 1:
            nu += [pair_sub(norms[k], norms[k - 1]), pair_sub(crosses[k], crosses[k - 1])]
        else:
            twice = pair_add(crosses[k - 1], crosses[k - 1])
            nu += [pair_sub(norms[k], norms[k - 1]), pair_sub(crosses[k], twice)]
    older, old = {}, dict(enumerate(nu))
    ratio = pair_div(old[1], old[0])
    diag, square = [ratio], []
    for k in range(1, STEPS):
        new = {}
        for l in range(k, 2 * STEPS - k):
            term = pair_sub(pair_add(old[l + 1], old[l - 1]), pair_mul(diag[-1], old[l]))
            if k > 1:
                term = pair_sub(term, pair_mul(square[-1], older[l]))
            new[l] = term
        square.append(pair_div(new[k], old[k - 1]))
        next_ratio = pair_div(new[k + 1], new[k])
        diag.append(pair_sub(next_ratio, ratio))
        ratio = next_ratio
        older, old = old, new
    return diag, square


def scaling(en_ref):
    energies = [en_ref[i] for i in range(en_ref.shape[0])]
    shift = sum(energies[1:], energies[0]) * (1.0 / len(energies))
    spread = sum((e - shift) * (e - shift) for e in energies) * (1.0 / len(energies))
    return energies, shift, spread + 6.0


def inverse_width(square, nx):
    return 1.0 / jnp.sqrt(jnp.full((1, nx), square, jnp.float32))


def iterate(
    n,
    group,
    sv_ref,
    lev_ref,
    en_ref,
    row_ref,
    basis,
    below,
    above,
    onsite,
    levels,
    stats,
    row_a,
    row_b,
    near,
    far,
    load_sem,
    met,
    up_send,
    up_recv,
    down_send,
    down_recv,
    near_send,
    near_recv,
    far_send,
    far_recv,
):
    ny, nx = onsite.shape
    rows = ny // CHUNKS
    block_rows = min(BLOCK, rows // 2)
    groups = n // group
    me = lax.axis_index("slab")
    up = lax.rem(me + 1, n)
    down = lax.rem(me + n - 1, n)
    mine = lax.rem(me, group)
    team = me // group

    def ring(d, size):
        return min(d, size - d)

    near_peers = []
    for d in sorted(range(1, group), key=lambda d: -ring(d, group)):
        place = lax.rem(mine + d, group)
        near_peers.append((place, team * group + place))
    long = min(8, groups)
    wide = groups // long
    far_peers = []
    steps = [(a, b) for a in range(wide) for b in range(long) if (a, b) != (0, 0)]
    for a, b in sorted(steps, key=lambda ab: -ring(ab[0], wide) - ring(ab[1], long)):
        place = lax.rem(team // long + a, wide) * long + lax.rem(team + b, long)
        far_peers.append((place, place * group + mine))

    def tell(sem, device):
        pl.semaphore_signal(sem, inc=1, device_id=(device,), device_id_type=MESH)

    barrier = pltpu.get_barrier_semaphore()
    tell(barrier, up)
    tell(barrier, down)

    def load(v, c):
        part = pl.ds(c * rows, rows)
        return pltpu.make_async_copy(
            sv_ref.at[v, 0, part], basis.at[1, v, part], load_sem.at[v * CHUNKS + c]
        )

    load_levels = pltpu.make_async_copy(lev_ref.at[0], levels, load_sem.at[2 * CHUNKS])
    for v in range(2):
        for c in range(CHUNKS):
            load(v, c).start()
    load_levels.start()

    pl.semaphore_wait(barrier, 2)

    rounds = n.bit_length() - 2

    def hear(r):
        pl.semaphore_wait(met.at[r - 1], 2)

    def say(r, distance):
        tell(met.at[r - 1], lax.rem(me + distance, n))
        tell(met.at[r - 1], lax.rem(me + n - distance, n))

    def halo(k, v, c, upward, half=False):
        part = pl.ds(c * rows, rows)
        if half:
            part = pl.ds(c * rows + (0 if upward else rows // 2), rows // 2)
        landing, send, recv, device = (
            (below, up_send, up_recv, up) if upward else (above, down_send, down_recv, down)
        )
        return pltpu.make_async_remote_copy(
            src_ref=basis.at[k + 1, v, part],
            dst_ref=landing.at[k, v, part],
            send_sem=send.at[k, v, c],
            recv_sem=recv.at[k, v, c],
            device_id=(device,),
            device_id_type=MESH,
        )

    for v in range(2):
        for c in range(CHUNKS):
            load(v, c).wait()
            halo(0, v, c, True).start()
            halo(0, v, c, False).start()

    energies, shift, square = scaling(en_ref)
    inv_row = inverse_width(square, nx)

    load_levels.wait()

    def fold(x):
        parts = [x[i : i + 8] for i in range(0, x.shape[0], 8)]
        while len(parts) > 1:
            parts = [a + b for a, b in zip(parts[::2], parts[1::2])]
        return parts[0]

    def place_onsite(b, carry):
        part = pl.ds(pl.multiple_of(b * block_rows, block_rows), block_rows)
        ids = levels[part, :]
        value = jnp.full((block_rows, nx), energies[0], jnp.float32)
        for i in range(1, len(energies)):
            value = jnp.where(ids == i, energies[i], value)
        onsite[part, :] = (value - shift) * inv_row
        out = []
        for v in range(2):
            basis[0, v, part, :] = jnp.zeros((block_rows, nx), jnp.float32)
            here = basis[1, v, part, :]
            h, e = two_sum(carry[v][0], fold(here * here))
            out.append((h, carry[v][1] + e))
        return tuple(out)

    def squeeze(total):
        h, l = total
        h, e = two_sum(h[:, :128], h[:, 128:])
        return h, (l[:, :128] + l[:, 128:]) + e

    zero_rows = jnp.zeros((8, nx), jnp.float32)
    none = (zero_rows, zero_rows)
    first_norms = lax.fori_loop(0, ny // block_rows, place_onsite, (none, none))
    for v in range(2):
        stats[4 * STEPS - 4 + v, 0], stats[4 * STEPS - 4 + v, 1] = squeeze(first_norms[v])

    def sweep(k, v, first, count, totals, landed=None):
        def block(b, carry):
            start = pl.multiple_of(first + b * block_rows, block_rows)
            part = pl.ds(start, block_rows)
            before = pl.ds(pl.multiple_of(lax.rem(start + (ny - 8), ny), 8), 8)
            after = pl.ds(pl.multiple_of(lax.rem(start + block_rows, ny), 8), 8)
            here = basis[k + 1, v, part, :]
            tall = jnp.concatenate(
                [basis[k + 1, v, before, :], here, basis[k + 1, v, after, :]], axis=0
            )
            height = block_rows + 16
            beside = pltpu.roll(tall, 1, 0)[8 : 8 + block_rows]
            beside = beside + pltpu.roll(tall, height - 1, 0)[8 : 8 + block_rows]
            beside = beside + (pltpu.roll(here, 1, 1) + pltpu.roll(here, nx - 1, 1))
            if landed is not None:
                one = landed[k, v, part, :]
                beside = beside + (one + one)
            else:
                beside = beside + (below[k, v, part, :] + above[k, v, part, :])
            new = onsite[part, :] * here - inv_row * beside
            out = []
            if landed is None:
                new = new - basis[k, v, part, :]
                basis[k + 2, v, part, :] = new
                out.append(new * new)
            out.append(new * here)
            added = []
            for (h, l), x in zip(carry, out):
                h, e = two_sum(h, fold(x))
                added.append((h, l + e))
            return tuple(added)

        return lax.fori_loop(0, count // block_rows, block, totals)

    sub = lax.broadcasted_iota(jnp.int32, (8, 128), 0)
    lane = lax.broadcasted_iota(jnp.int32, (8, 128), 1)

    def lane_sums(items):
        high = jnp.zeros((8, 128), jnp.float32)
        low = jnp.zeros((8, 128), jnp.float32)
        target = jnp.full((8, 128), 1000, jnp.int32)
        for q, (h, l, place) in enumerate(items):
            for shift_by in (4, 2, 1):
                h, e = two_sum(h, pltpu.roll(h, shift_by, 0))
                l = l + pltpu.roll(l, shift_by, 0) + e
            high = jnp.where(sub == q, h, high)
            low = jnp.where(sub == q, l, low)
            target = jnp.where(sub == q, place, target)
        for shift_by in (64, 32, 16, 8, 4, 2, 1):
            high, e = two_sum(high, pltpu.roll(high, shift_by, 1))
            low = low + pltpu.roll(low, shift_by, 1) + e
        return jnp.where(lane == target, high, 0.0) + jnp.where(
            lane == target + 16, low, 0.0
        )

    def step(k, final_sends=False):
        for v in range(2):
            totals = (none, none)
            for c in range(CHUNKS):
                halo(k, v, c, True).wait_recv()
                halo(k, v, c, False).wait_recv()
                totals = sweep(k, v, c * rows, rows, totals)
                halo(k + 1, v, c, True, final_sends).start()
                halo(k + 1, v, c, False, final_sends).start()
            for q in range(2):
                stats[4 * k + 2 * v + q, 0], stats[4 * k + 2 * v + q, 1] = squeeze(totals[q])

    def last_step():
        k = STEPS - 1
        ends = []
        for v in range(2):
            totals = (none,)
            for c in range(CHUNKS):
                if v == 1 and c == CHUNKS - 1:
                    places = [64 * (i % 4 // 2) + (8 + i // 4 if i % 2 else 1 + i // 4) for i in range(4 * k)]
                    places += [0, 64]
                    packed = jnp.zeros((8, 128), jnp.float32)
                    for i in range(0, len(places), 8):
                        packed = packed + lane_sums(
                            [(stats[j, 0], stats[j, 1], places[j]) for j in range(i, min(i + 8, len(places)))]
                        )
                halo(k, v, c, True, True).wait_recv()
                halo(k, v, c, False, True).wait_recv()
                totals = sweep(k, v, c * rows, rows // 2, totals, below)
                totals = sweep(k, v, c * rows + rows // 2, rows // 2, totals, above)
            ends.append(squeeze(totals[0]))
        return packed + lane_sums([(h, l, 64 * v + 8 + k) for v, (h, l) in enumerate(ends)])

    say(1, 1)
    step(0)

    def middle(k, distance):
        @pl.when(k <= rounds)
        def _():
            hear(k)

        @pl.when(k < rounds)
        def _():
            say(k + 1, distance)

        step(k)
        return distance * 2

    lax.fori_loop(1, STEPS - 2, middle, 2)
    for k in (STEPS - 2, STEPS - 1):
        if k <= rounds:
            hear(k)
        if k < rounds:
            say(k + 1, 2**k)
        if k == STEPS - 2:
            step(k, final_sends=True)
    packed = last_step()
    if rounds == STEPS:
        hear(rounds)

    for shift_by in (4, 2, 1):
        packed = packed + pltpu.roll(packed, shift_by, 0)

    row_lane = lax.broadcasted_iota(jnp.int32, (1, 128), 1)
    is_high = lax.rem(row_lane, 64) < 16

    def exchange(row, staging, slots, place, peers, send, recv):
        def copy(i, slot):
            return pltpu.make_async_remote_copy(
                src_ref=staging,
                dst_ref=slots.at[slot],
                send_sem=send.at[i],
                recv_sem=recv.at[slot],
                device_id=(peers[i][1],),
                device_id_type=MESH,
            )

        staging[...] = row
        slots[place] = row
        for i in range(len(peers)):
            copy(i, place).start()
        for i in reversed(range(len(peers))):
            copy(i, peers[i][0]).wait_recv()
        total, lost = tree_rows([slots[i] for i in range(len(peers) + 1)])
        return jnp.where(is_high, total, total + pltpu.roll(lost, 16, 1)), [
            copy(i, place) for i in range(len(peers))
        ]

    row, sent = exchange(packed[0:1], row_a, near, mine, near_peers, near_send, near_recv)
    row, more = exchange(row, row_b, far, team, far_peers, far_send, far_recv)
    row = jnp.where(row_lane == 40, shift, row)
    row = jnp.where(row_lane == 41, inv_row[:, :128], row)
    row_ref[...] = row
    for copy in sent + more:
        copy.wait_send()

    def drain(k, _):
        for v in range(2):
            for c in range(CHUNKS):
                halo(k, v, c, True).wait_send()
                halo(k, v, c, False).wait_send()
        return None

    lax.fori_loop(0, STEPS - 1, drain, None)
    for v in range(2):
        for c in range(CHUNKS):
            halo(STEPS - 1, v, c, True, True).wait_send()
            halo(STEPS - 1, v, c, False, True).wait_send()


def combine(
    row_ref,
    basis,
    field_ref,
    diag_ref,
    off_ref,
    mom_ref,
    field,
    table,
    out_sem,
):
    ny, nx = field.shape[1:]

    row = row_ref[...]
    row_lane = lax.broadcasted_iota(jnp.int32, (1, 128), 1)
    shift = jnp.sum(jnp.where(row_lane == 40, row, 0.0), axis=1, keepdims=True)
    inv_row = jnp.sum(jnp.where(row_lane == 41, row, 0.0), axis=1, keepdims=True)
    tall_row = lax.broadcasted_iota(jnp.int32, (32, 128), 0)
    tall_lane = lax.broadcasted_iota(jnp.int32, (32, 128), 1)
    spread_row = jnp.broadcast_to(row, (32, 128))
    first = jnp.sum(jnp.where(tall_lane == tall_row, spread_row, 0.0), axis=1, keepdims=True)
    second = jnp.sum(
        jnp.where(tall_lane == tall_row + 64, spread_row, 0.0), axis=1, keepdims=True
    )
    table[...] = jnp.where(tall_lane < 64, first, second)

    norms = [(table[k : k + 1, :], table[16 + k : 17 + k, :]) for k in range(STEPS)]
    crosses = [(table[8 + k : 9 + k, :], table[24 + k : 25 + k, :]) for k in range(STEPS)]
    diag, square = coefficients(norms, crosses)

    width = jnp.broadcast_to(1.0 / inv_row, (1, 128))
    alphas = [shift + width * a[0] for a in diag]
    betas = [width * jnp.sqrt(b[0]) for b in square]
    zero = jnp.zeros((1, 128), jnp.float32)
    left = [zero] + betas
    right = betas + [zero]
    emin = functools.reduce(jnp.minimum, [a - p - q for a, p, q in zip(alphas, left, right)])
    emax = functools.reduce(jnp.maximum, [a + p + q for a, p, q in zip(alphas, left, right)])
    center = (emax + emin) * 0.5
    inv_half = 1.0 / (0.55 * (emax - emin))
    slope = width * inv_half
    offset = (shift - center) * inv_half

    def apply(poly):
        around = [zero] + poly + [zero]
        out = []
        for k in range(len(poly) + 1):
            value = slope * around[k] if k else None
            if k < len(poly):
                value = offset * poly[k] if value is None else value + offset * poly[k]
            if k + 2 < len(around) - 1:
                value = value + slope * around[k + 2]
            out.append(value)
        return out

    t0 = [zero + 1.0]
    t1 = apply(t0)
    t2 = [2.0 * q for q in apply(t1)]
    t2[0] = t2[0] - 1.0
    t3 = [2.0 * q for q in apply(t2)]
    t3 = [q - t1[k] if k < 2 else q for k, q in enumerate(t3)]

    inv_norm = 1.0 / norms[0][0]
    size = [q[0] * inv_norm for q in norms[:4]]
    cross = [q[0] * inv_norm for q in crosses[:3]]
    skip = pair_sub(norms[1], norms[0])[0] * inv_norm
    skip_next = pair_sub(norms[2], norms[0])[0] * inv_norm
    skip_two = pair_sub(crosses[1], crosses[0])[0] * inv_norm
    gram = [
        [zero + 1.0, cross[0], skip, skip_two],
        [cross[0], size[1], cross[1], skip_next],
        [skip, cross[1], size[2], cross[2]],
        [skip_two, skip_next, cross[2], size[3]],
    ]

    def inner(p, q):
        return sum(
            a * sum(b * gram[i][j] for j, b in enumerate(q)) for i, a in enumerate(p)
        )

    d01 = inner(t0, t1)
    moments = [
        d01,
        inner(t0, t2),
        inner(t0, t3),
        2.0 * inner(t2, t2) - 1.0,
        2.0 * inner(t3, t2) - d01,
        2.0 * inner(t3, t3) - 1.0,
    ]

    def emit(ref, values):
        packed = zero
        for k, value in enumerate(values):
            packed = jnp.where(lax.rem(row_lane, 64) == k, value, packed)
        ref[0:1, :] = packed[:, : len(values)]
        ref[1:2, :] = pltpu.roll(packed, 64, 1)[:, : len(values)]

    half = ny // 2

    def store(v, i):
        part = pl.ds(i * half, half)
        return pltpu.make_async_copy(
            field.at[v, part], field_ref.at[v, 0, part], out_sem.at[v, i]
        )

    for v in range(2):
        own = row_lane < 64 if v == 0 else row_lane >= 64
        scale = [jnp.where(own, q, pltpu.roll(q, 64, 1)) for q in t3]
        scale = [jnp.concatenate([q, q], axis=1) for q in scale]
        for i in range(2):

            def finish(b, _):
                part = pl.ds(pl.multiple_of(i * half + b * BLOCK, BLOCK), BLOCK)
                value = scale[0] * basis[1, v, part, :] + scale[1] * basis[2, v, part, :]
                value = value + scale[2] * basis[3, v, part, :]
                field[v, part, :] = value + scale[3] * basis[4, v, part, :]
                return None

            lax.fori_loop(0, half // BLOCK, finish, None)
            store(v, i).start()

    emit(diag_ref, alphas)
    emit(off_ref, betas)
    emit(mom_ref, moments)
    for v in range(2):
        for i in range(2):
            store(v, i).wait()


def solution(mesh):
    n = mesh.shape["slab"]
    group = 16 if n >= 128 else 4

    def shards(start_vectors, levels, energies):
        vecs, _, ny, nx = start_vectors.shape
        f32 = jnp.float32
        dma = pltpu.SemaphoreType.DMA
        vmem = pl.BlockSpec(memory_space=pltpu.VMEM)
        hbm = pl.BlockSpec(memory_space=pltpu.HBM)
        halo_sem = dma((STEPS, vecs, CHUNKS))
        smem = pl.BlockSpec(memory_space=pltpu.SMEM)
        groups = n // group
        row, basis = pl.pallas_call(
            functools.partial(iterate, n, group),
            out_shape=(
                pltpu.VMEM((1, 128), f32),
                pltpu.VMEM((STEPS + 1, vecs, ny, nx), f32),
            ),
            in_specs=[hbm, hbm, smem],
            out_specs=(vmem, vmem),
            scratch_shapes=[
                pltpu.VMEM((STEPS, vecs, ny, nx), f32),
                pltpu.VMEM((STEPS, vecs, ny, nx), f32),
                pltpu.VMEM((ny, nx), f32),
                pltpu.VMEM((ny, nx), jnp.int32),
                pltpu.VMEM((4 * STEPS - 2, 2, 8, 128), f32),
                pltpu.VMEM((1, 128), f32),
                pltpu.VMEM((1, 128), f32),
                pltpu.VMEM((group, 1, 128), f32),
                pltpu.VMEM((groups, 1, 128), f32),
                dma((2 * CHUNKS + 1,)),
                pltpu.SemaphoreType.REGULAR((STEPS,)),
                halo_sem,
                halo_sem,
                halo_sem,
                halo_sem,
                dma((group,)),
                dma((group,)),
                dma((groups,)),
                dma((groups,)),
            ],
            compiler_params=pltpu.CompilerParams(
                collective_id=0, has_side_effects=True, vmem_limit_bytes=62_000_000
            ),
        )(start_vectors, levels, energies)
        return pl.pallas_call(
            combine,
            out_shape=(
                jax.ShapeDtypeStruct(start_vectors.shape, f32),
                jax.ShapeDtypeStruct((vecs, STEPS), f32),
                jax.ShapeDtypeStruct((vecs, STEPS - 1), f32),
                jax.ShapeDtypeStruct((vecs, 6), f32),
            ),
            in_specs=[vmem, vmem],
            out_specs=(hbm, vmem, vmem, vmem),
            scratch_shapes=[
                pltpu.VMEM((vecs, ny, nx), f32),
                pltpu.VMEM((32, 128), f32),
                dma((vecs, 2)),
            ],
            compiler_params=pltpu.CompilerParams(vmem_limit_bytes=8 * 2**20),
        )(row, basis)

    return jax.shard_map(
        shards,
        mesh=mesh,
        in_specs=(P(None, "slab", None, None), P("slab", None, None), P()),
        out_specs=(P(None, "slab", None, None), P(), P(), P()),
        check_vma=False,
    )
```

```python
import functools

import jax
import jax.numpy as jnp
from jax import lax
from jax.experimental import pallas as pl
from jax.experimental.pallas import tpu as pltpu
from jax.sharding import PartitionSpec as P

STEPS = 8
CHUNKS = 4
BLOCK = 32
MESH = pl.DeviceIdType.MESH


def two_sum(a, b):
    s = a + b
    t = s - a
    return s, (a - (s - t)) + (b - t)


def fast_two_sum(a, b):
    s = a + b
    return s, b - (s - a)


def split(a):
    t = a * 4097.0
    high = t - (t - a)
    return high, a - high


def two_prod(a, b):
    p = a * b
    ah, al = split(a)
    bh, bl = split(b)
    return p, ((ah * bh - p) + ah * bl + al * bh) + al * bl


def pair_add(a, b):
    s, e = two_sum(a[0], b[0])
    return fast_two_sum(s, e + (a[1] + b[1]))


def pair_neg(a):
    return -a[0], -a[1]


def pair_sub(a, b):
    return pair_add(a, pair_neg(b))


def pair_mul(a, b):
    p, e = two_prod(a[0], b[0])
    return fast_two_sum(p, e + (a[0] * b[1] + a[1] * b[0]))


def pair_div(a, b):
    inv = 1.0 / b[0]
    first = a[0] * inv
    p, e = two_prod(first, b[0])
    rest = (a[0] - p) - e + a[1] - first * b[1]
    return fast_two_sum(first, rest * inv)


def tree_rows(rows):
    lost = None
    while len(rows) > 1:
        sums = []
        for a, b in zip(rows[::2], rows[1::2]):
            s, e = two_sum(a, b)
            sums.append(s)
            lost = e if lost is None else lost + e
        rows = sums
    return rows[0], lost


def coefficients(norms, crosses):
    nu = []
    for k in range(STEPS):
        if k == 0:
            nu += [norms[0], crosses[0]]
        elif k < STEPS - 1:
            nu += [pair_sub(norms[k], norms[k - 1]), pair_sub(crosses[k], crosses[k - 1])]
        else:
            twice = pair_add(crosses[k - 1], crosses[k - 1])
            nu += [pair_sub(norms[k], norms[k - 1]), pair_sub(crosses[k], twice)]
    older, old = {}, dict(enumerate(nu))
    ratio = pair_div(old[1], old[0])
    diag, square = [ratio], []
    for k in range(1, STEPS):
        new = {}
        for l in range(k, 2 * STEPS - k):
            term = pair_sub(pair_add(old[l + 1], old[l - 1]), pair_mul(diag[-1], old[l]))
            if k > 1:
                term = pair_sub(term, pair_mul(square[-1], older[l]))
            new[l] = term
        square.append(pair_div(new[k], old[k - 1]))
        next_ratio = pair_div(new[k + 1], new[k])
        diag.append(pair_sub(next_ratio, ratio))
        ratio = next_ratio
        older, old = old, new
    return diag, square


def scaling(en_ref):
    energies = [en_ref[i] for i in range(en_ref.shape[0])]
    shift = sum(energies[1:], energies[0]) * (1.0 / len(energies))
    spread = sum((e - shift) * (e - shift) for e in energies) * (1.0 / len(energies))
    return energies, shift, spread + 6.0


def inverse_width(square, nx):
    return 1.0 / jnp.sqrt(jnp.full((1, nx), square, jnp.float32))


def iterate(
    n,
    group,
    sv_ref,
    lev_ref,
    en_ref,
    row_ref,
    basis,
    below,
    above,
    onsite,
    levels,
    stats,
    row_a,
    row_b,
    near,
    far,
    load_sem,
    met,
    up_send,
    up_recv,
    down_send,
    down_recv,
    near_send,
    near_recv,
    far_send,
    far_recv,
):
    ny, nx = onsite.shape
    rows = ny // CHUNKS
    block_rows = min(BLOCK, rows // 2)
    groups = n // group
    me = lax.axis_index("slab")
    up = lax.rem(me + 1, n)
    down = lax.rem(me + n - 1, n)
    mine = lax.rem(me, group)
    team = me // group

    def ring(d, size):
        return min(d, size - d)

    near_peers = []
    for d in sorted(range(1, group), key=lambda d: -ring(d, group)):
        place = lax.rem(mine + d, group)
        near_peers.append((place, team * group + place))
    long = min(8, groups)
    wide = groups // long
    far_peers = []
    steps = [(a, b) for a in range(wide) for b in range(long) if (a, b) != (0, 0)]
    for a, b in sorted(steps, key=lambda ab: -ring(ab[0], wide) - ring(ab[1], long)):
        place = lax.rem(team // long + a, wide) * long + lax.rem(team + b, long)
        far_peers.append((place, place * group + mine))

    def tell(sem, device):
        pl.semaphore_signal(sem, inc=1, device_id=(device,), device_id_type=MESH)

    barrier = pltpu.get_barrier_semaphore()
    tell(barrier, up)
    tell(barrier, down)

    def load(v, c):
        part = pl.ds(c * rows, rows)
        return pltpu.make_async_copy(
            sv_ref.at[v, 0, part], basis.at[1, v, part], load_sem.at[v * CHUNKS + c]
        )

    load_levels = pltpu.make_async_copy(lev_ref.at[0], levels, load_sem.at[2 * CHUNKS])
    for v in range(2):
        for c in range(CHUNKS):
            load(v, c).start()
    load_levels.start()

    pl.semaphore_wait(barrier, 2)

    rounds = n.bit_length() - 2

    def hear(r):
        pl.semaphore_wait(met.at[r - 1], 2)

    def say(r, distance):
        tell(met.at[r - 1], lax.rem(me + distance, n))
        tell(met.at[r - 1], lax.rem(me + n - distance, n))

    def halo(k, v, c, upward, half=False):
        part = pl.ds(c * rows, rows)
        if half:
            part = pl.ds(c * rows + (0 if upward else rows // 2), rows // 2)
        landing, send, recv, device = (
            (below, up_send, up_recv, up) if upward else (above, down_send, down_recv, down)
        )
        return pltpu.make_async_remote_copy(
            src_ref=basis.at[k + 1, v, part],
            dst_ref=landing.at[k, v, part],
            send_sem=send.at[k, v, c],
            recv_sem=recv.at[k, v, c],
            device_id=(device,),
            device_id_type=MESH,
        )

    for v in range(2):
        for c in range(CHUNKS):
            load(v, c).wait()
            halo(0, v, c, True).start()
            halo(0, v, c, False).start()

    energies, shift, square = scaling(en_ref)
    inv_row = inverse_width(square, nx)

    load_levels.wait()

    def fold(x):
        parts = [x[i : i + 8] for i in range(0, x.shape[0], 8)]
        while len(parts) > 1:
            parts = [a + b for a, b in zip(parts[::2], parts[1::2])]
        return parts[0]

    def place_onsite(b, carry):
        part = pl.ds(pl.multiple_of(b * block_rows, block_rows), block_rows)
        ids = levels[part, :]
        value = jnp.full((block_rows, nx), energies[0], jnp.float32)
        for i in range(1, len(energies)):
            value = jnp.where(ids == i, energies[i], value)
        onsite[part, :] = (value - shift) * inv_row
        out = []
        for v in range(2):
            basis[0, v, part, :] = jnp.zeros((block_rows, nx), jnp.float32)
            here = basis[1, v, part, :]
            h, e = two_sum(carry[v][0], fold(here * here))
            out.append((h, carry[v][1] + e))
        return tuple(out)

    def squeeze(total):
        h, l = total
        h, e = two_sum(h[:, :128], h[:, 128:])
        return h, (l[:, :128] + l[:, 128:]) + e

    zero_rows = jnp.zeros((8, nx), jnp.float32)
    none = (zero_rows, zero_rows)
    first_norms = lax.fori_loop(0, ny // block_rows, place_onsite, (none, none))
    for v in range(2):
        stats[4 * STEPS - 4 + v, 0], stats[4 * STEPS - 4 + v, 1] = squeeze(first_norms[v])

    def sweep(k, v, first, count, totals, landed=None):
        def block(b, carry):
            start = pl.multiple_of(first + b * block_rows, block_rows)
            part = pl.ds(start, block_rows)
            before = pl.ds(pl.multiple_of(lax.rem(start + (ny - 8), ny), 8), 8)
            after = pl.ds(pl.multiple_of(lax.rem(start + block_rows, ny), 8), 8)
            here = basis[k + 1, v, part, :]
            tall = jnp.concatenate(
                [basis[k + 1, v, before, :], here, basis[k + 1, v, after, :]], axis=0
            )
            height = block_rows + 16
            beside = pltpu.roll(tall, 1, 0)[8 : 8 + block_rows]
            beside = beside + pltpu.roll(tall, height - 1, 0)[8 : 8 + block_rows]
            beside = beside + (pltpu.roll(here, 1, 1) + pltpu.roll(here, nx - 1, 1))
            if landed is not None:
                one = landed[k, v, part, :]
                beside = beside + (one + one)
            else:
                beside = beside + (below[k, v, part, :] + above[k, v, part, :])
            new = onsite[part, :] * here - inv_row * beside
            out = []
            if landed is None:
                new = new - basis[k, v, part, :]
                basis[k + 2, v, part, :] = new
                out.append(new * new)
            out.append(new * here)
            added = []
            for (h, l), x in zip(carry, out):
                h, e = two_sum(h, fold(x))
                added.append((h, l + e))
            return tuple(added)

        return lax.fori_loop(0, count // block_rows, block, totals)

    sub = lax.broadcasted_iota(jnp.int32, (8, 128), 0)
    lane = lax.broadcasted_iota(jnp.int32, (8, 128), 1)

    def lane_sums(items):
        high = jnp.zeros((8, 128), jnp.float32)
        low = jnp.zeros((8, 128), jnp.float32)
        target = jnp.full((8, 128), 1000, jnp.int32)
        for q, (h, l, place) in enumerate(items):
            for shift_by in (4, 2, 1):
                h, e = two_sum(h, pltpu.roll(h, shift_by, 0))
                l = l + pltpu.roll(l, shift_by, 0) + e
            high = jnp.where(sub == q, h, high)
            low = jnp.where(sub == q, l, low)
            target = jnp.where(sub == q, place, target)
        for shift_by in (64, 32, 16, 8, 4, 2, 1):
            high, e = two_sum(high, pltpu.roll(high, shift_by, 1))
            low = low + pltpu.roll(low, shift_by, 1) + e
        return jnp.where(lane == target, high, 0.0) + jnp.where(
            lane == target + 16, low, 0.0
        )

    def step(k, final_sends=False):
        for v in range(2):
            totals = (none, none)
            for c in range(CHUNKS):
                halo(k, v, c, True).wait_recv()
                halo(k, v, c, False).wait_recv()
                totals = sweep(k, v, c * rows, rows, totals)
                halo(k + 1, v, c, True, final_sends).start()
                halo(k + 1, v, c, False, final_sends).start()
            for q in range(2):
                stats[4 * k + 2 * v + q, 0], stats[4 * k + 2 * v + q, 1] = squeeze(totals[q])

    def last_step():
        k = STEPS - 1
        ends = []
        for v in range(2):
            totals = (none,)
            for c in range(CHUNKS):
                if v == 1 and c == CHUNKS - 1:
                    places = [64 * (i % 4 // 2) + (8 + i // 4 if i % 2 else 1 + i // 4) for i in range(4 * k)]
                    places += [0, 64]
                    packed = jnp.zeros((8, 128), jnp.float32)
                    for i in range(0, len(places), 8):
                        packed = packed + lane_sums(
                            [(stats[j, 0], stats[j, 1], places[j]) for j in range(i, min(i + 8, len(places)))]
                        )
                halo(k, v, c, True, True).wait_recv()
                halo(k, v, c, False, True).wait_recv()
                totals = sweep(k, v, c * rows, rows // 2, totals, below)
                totals = sweep(k, v, c * rows + rows // 2, rows // 2, totals, above)
            ends.append(squeeze(totals[0]))
        return packed + lane_sums([(h, l, 64 * v + 8 + k) for v, (h, l) in enumerate(ends)])

    say(1, 1)
    step(0)

    def middle(k, distance):
        @pl.when(k <= rounds)
        def _():
            hear(k)

        @pl.when(k < rounds)
        def _():
            say(k + 1, distance)

        step(k)
        return distance * 2

    lax.fori_loop(1, STEPS - 2, middle, 2)
    for k in (STEPS - 2, STEPS - 1):
        if k <= rounds:
            hear(k)
        if k < rounds:
            say(k + 1, 2**k)
        if k == STEPS - 2:
            step(k, final_sends=True)
    packed = last_step()
    if rounds == STEPS:
        hear(rounds)

    for shift_by in (4, 2, 1):
        packed = packed + pltpu.roll(packed, shift_by, 0)

    row_lane = lax.broadcasted_iota(jnp.int32, (1, 128), 1)
    is_high = lax.rem(row_lane, 64) < 16

    def drain(k, _):
        for v in range(2):
            for c in range(CHUNKS):
                halo(k, v, c, True).wait_send()
                halo(k, v, c, False).wait_send()
        return None

    def drain_all():
        lax.fori_loop(0, STEPS - 1, drain, None)
        for v in range(2):
            for c in range(CHUNKS):
                halo(STEPS - 1, v, c, True, True).wait_send()
                halo(STEPS - 1, v, c, False, True).wait_send()

    def exchange(row, staging, slots, place, peers, send, recv, meanwhile):
        def copy(i, slot):
            return pltpu.make_async_remote_copy(
                src_ref=staging,
                dst_ref=slots.at[slot],
                send_sem=send.at[i],
                recv_sem=recv.at[slot],
                device_id=(peers[i][1],),
                device_id_type=MESH,
            )

        staging[...] = row
        slots[place] = row
        for i in range(len(peers)):
            copy(i, place).start()
        meanwhile()
        for i in reversed(range(len(peers))):
            copy(i, peers[i][0]).wait_recv()
        total, lost = tree_rows([slots[i] for i in range(len(peers) + 1)])
        return jnp.where(is_high, total, total + pltpu.roll(lost, 16, 1)), [
            copy(i, place) for i in range(len(peers))
        ]

    row, sent = exchange(packed[0:1], row_a, near, mine, near_peers, near_send, near_recv, drain_all)

    def drain_near():
        for copy in sent:
            copy.wait_send()

    row, more = exchange(
        row, row_b, far, team, far_peers, far_send, far_recv, drain_near
    )
    row = jnp.where(row_lane == 40, shift, row)
    row = jnp.where(row_lane == 41, inv_row[:, :128], row)
    row_ref[...] = row
    for copy in more:
        copy.wait_send()


def combine(
    row_ref,
    basis,
    field_ref,
    diag_ref,
    off_ref,
    mom_ref,
    field,
    diag_out,
    off_out,
    mom_out,
    table,
    out_sem,
    small_sem,
):
    ny, nx = field.shape[1:]

    row = row_ref[...]
    row_lane = lax.broadcasted_iota(jnp.int32, (1, 128), 1)
    shift = jnp.sum(jnp.where(row_lane == 40, row, 0.0), axis=1, keepdims=True)
    inv_row = jnp.sum(jnp.where(row_lane == 41, row, 0.0), axis=1, keepdims=True)
    tall_row = lax.broadcasted_iota(jnp.int32, (32, 128), 0)
    tall_lane = lax.broadcasted_iota(jnp.int32, (32, 128), 1)
    spread_row = jnp.broadcast_to(row, (32, 128))
    first = jnp.sum(jnp.where(tall_lane == tall_row, spread_row, 0.0), axis=1, keepdims=True)
    second = jnp.sum(
        jnp.where(tall_lane == tall_row + 64, spread_row, 0.0), axis=1, keepdims=True
    )
    table[...] = jnp.where(tall_lane < 64, first, second)

    norms = [(table[k : k + 1, :], table[16 + k : 17 + k, :]) for k in range(STEPS)]
    crosses = [(table[8 + k : 9 + k, :], table[24 + k : 25 + k, :]) for k in range(STEPS)]
    diag, square = coefficients(norms, crosses)

    width = jnp.broadcast_to(1.0 / inv_row, (1, 128))
    alphas = [shift + width * a[0] for a in diag]
    betas = [width * jnp.sqrt(b[0]) for b in square]
    zero = jnp.zeros((1, 128), jnp.float32)
    left = [zero] + betas
    right = betas + [zero]
    emin = functools.reduce(jnp.minimum, [a - p - q for a, p, q in zip(alphas, left, right)])
    emax = functools.reduce(jnp.maximum, [a + p + q for a, p, q in zip(alphas, left, right)])
    center = (emax + emin) * 0.5
    inv_half = 1.0 / (0.55 * (emax - emin))
    slope = width * inv_half
    offset = (shift - center) * inv_half

    def apply(poly):
        around = [zero] + poly + [zero]
        out = []
        for k in range(len(poly) + 1):
            value = slope * around[k] if k else None
            if k < len(poly):
                value = offset * poly[k] if value is None else value + offset * poly[k]
            if k + 2 < len(around) - 1:
                value = value + slope * around[k + 2]
            out.append(value)
        return out

    t0 = [zero + 1.0]
    t1 = apply(t0)
    t2 = [2.0 * q for q in apply(t1)]
    t2[0] = t2[0] - 1.0
    t3 = [2.0 * q for q in apply(t2)]
    t3 = [q - t1[k] if k < 2 else q for k, q in enumerate(t3)]

    inv_norm = 1.0 / norms[0][0]
    size = [q[0] * inv_norm for q in norms[:4]]
    cross = [q[0] * inv_norm for q in crosses[:3]]
    skip = pair_sub(norms[1], norms[0])[0] * inv_norm
    skip_next = pair_sub(norms[2], norms[0])[0] * inv_norm
    skip_two = pair_sub(crosses[1], crosses[0])[0] * inv_norm
    gram = [
        [zero + 1.0, cross[0], skip, skip_two],
        [cross[0], size[1], cross[1], skip_next],
        [skip, cross[1], size[2], cross[2]],
        [skip_two, skip_next, cross[2], size[3]],
    ]

    def inner(p, q):
        return sum(
            a * sum(b * gram[i][j] for j, b in enumerate(q)) for i, a in enumerate(p)
        )

    d01 = inner(t0, t1)
    moments = [
        d01,
        inner(t0, t2),
        inner(t0, t3),
        2.0 * inner(t2, t2) - 1.0,
        2.0 * inner(t3, t2) - d01,
        2.0 * inner(t3, t3) - 1.0,
    ]

    def emit(ref, values):
        packed = zero
        for k, value in enumerate(values):
            packed = jnp.where(lax.rem(row_lane, 64) == k, value, packed)
        ref[0:1, :] = packed[:, : len(values)]
        ref[1:2, :] = pltpu.roll(packed, 64, 1)[:, : len(values)]

    small = []
    for k, (stage, ref, values) in enumerate(
        [(diag_out, diag_ref, alphas), (off_out, off_ref, betas), (mom_out, mom_ref, moments)]
    ):
        emit(stage, values)
        small.append(pltpu.make_async_copy(stage, ref, small_sem.at[k]))

    half = ny // 4

    def store(v, i):
        part = pl.ds(i * half, half)
        return pltpu.make_async_copy(
            field.at[v, part], field_ref.at[v, 0, part], out_sem.at[v, i]
        )

    for v in range(2):
        own = row_lane < 64 if v == 0 else row_lane >= 64
        scale = [jnp.where(own, q, pltpu.roll(q, 64, 1)) for q in t3]
        scale = [jnp.concatenate([q, q], axis=1) for q in scale]
        for i in range(4):

            def finish(b, _):
                part = pl.ds(pl.multiple_of(i * half + b * BLOCK, BLOCK), BLOCK)
                value = scale[0] * basis[1, v, part, :] + scale[1] * basis[2, v, part, :]
                value = value + scale[2] * basis[3, v, part, :]
                field[v, part, :] = value + scale[3] * basis[4, v, part, :]
                return None

            lax.fori_loop(0, half // BLOCK, finish, None)
            store(v, i).start()
        if v == 0:
            for copy in small:
                copy.start()

    for v in range(2):
        for i in range(4):
            store(v, i).wait()
    for copy in small:
        copy.wait()


def solution(mesh):
    n = mesh.shape["slab"]
    group = 16 if n >= 128 else 4

    def shards(start_vectors, levels, energies):
        vecs, _, ny, nx = start_vectors.shape
        f32 = jnp.float32
        dma = pltpu.SemaphoreType.DMA
        vmem = pl.BlockSpec(memory_space=pltpu.VMEM)
        hbm = pl.BlockSpec(memory_space=pltpu.HBM)
        halo_sem = dma((STEPS, vecs, CHUNKS))
        smem = pl.BlockSpec(memory_space=pltpu.SMEM)
        groups = n // group
        row, basis = pl.pallas_call(
            functools.partial(iterate, n, group),
            out_shape=(
                pltpu.VMEM((1, 128), f32),
                pltpu.VMEM((STEPS + 1, vecs, ny, nx), f32),
            ),
            in_specs=[hbm, hbm, smem],
            out_specs=(vmem, vmem),
            scratch_shapes=[
                pltpu.VMEM((STEPS, vecs, ny, nx), f32),
                pltpu.VMEM((STEPS, vecs, ny, nx), f32),
                pltpu.VMEM((ny, nx), f32),
                pltpu.VMEM((ny, nx), jnp.int32),
                pltpu.VMEM((4 * STEPS - 2, 2, 8, 128), f32),
                pltpu.VMEM((1, 128), f32),
                pltpu.VMEM((1, 128), f32),
                pltpu.VMEM((group, 1, 128), f32),
                pltpu.VMEM((groups, 1, 128), f32),
                dma((2 * CHUNKS + 1,)),
                pltpu.SemaphoreType.REGULAR((STEPS,)),
                halo_sem,
                halo_sem,
                halo_sem,
                halo_sem,
                dma((group,)),
                dma((group,)),
                dma((groups,)),
                dma((groups,)),
            ],
            compiler_params=pltpu.CompilerParams(
                collective_id=0, has_side_effects=True, vmem_limit_bytes=62_000_000
            ),
        )(start_vectors, levels, energies)
        return pl.pallas_call(
            combine,
            out_shape=(
                jax.ShapeDtypeStruct(start_vectors.shape, f32),
                jax.ShapeDtypeStruct((vecs, STEPS), f32),
                jax.ShapeDtypeStruct((vecs, STEPS - 1), f32),
                jax.ShapeDtypeStruct((vecs, 6), f32),
            ),
            in_specs=[vmem, vmem],
            out_specs=(hbm, hbm, hbm, hbm),
            scratch_shapes=[
                pltpu.VMEM((vecs, ny, nx), f32),
                pltpu.VMEM((vecs, STEPS), f32),
                pltpu.VMEM((vecs, STEPS - 1), f32),
                pltpu.VMEM((vecs, 6), f32),
                pltpu.VMEM((32, 128), f32),
                dma((vecs, 4)),
                dma((3,)),
            ],
            compiler_params=pltpu.CompilerParams(vmem_limit_bytes=8 * 2**20),
        )(row, basis)

    return jax.shard_map(
        shards,
        mesh=mesh,
        in_specs=(P(None, "slab", None, None), P("slab", None, None), P()),
        out_specs=(P(None, "slab", None, None), P(), P(), P()),
        check_vma=False,
    )
```

```python
import functools

import jax
import jax.numpy as jnp
from jax import lax
from jax.experimental import pallas as pl
from jax.experimental.pallas import tpu as pltpu
from jax.sharding import PartitionSpec as P

STEPS = 8
CHUNKS = 4
BLOCK = 32
MESH = pl.DeviceIdType.MESH


def two_sum(a, b):
    s = a + b
    t = s - a
    return s, (a - (s - t)) + (b - t)


def fast_two_sum(a, b):
    s = a + b
    return s, b - (s - a)


def split(a):
    t = a * 4097.0
    high = t - (t - a)
    return high, a - high


def two_prod(a, b):
    p = a * b
    ah, al = split(a)
    bh, bl = split(b)
    return p, ((ah * bh - p) + ah * bl + al * bh) + al * bl


def pair_add(a, b):
    s, e = two_sum(a[0], b[0])
    return fast_two_sum(s, e + (a[1] + b[1]))


def pair_neg(a):
    return -a[0], -a[1]


def pair_sub(a, b):
    return pair_add(a, pair_neg(b))


def pair_mul(a, b):
    p, e = two_prod(a[0], b[0])
    return fast_two_sum(p, e + (a[0] * b[1] + a[1] * b[0]))


def pair_div(a, b):
    inv = 1.0 / b[0]
    first = a[0] * inv
    p, e = two_prod(first, b[0])
    rest = (a[0] - p) - e + a[1] - first * b[1]
    return fast_two_sum(first, rest * inv)


def tree_rows(rows):
    lost = None
    while len(rows) > 1:
        sums = []
        for a, b in zip(rows[::2], rows[1::2]):
            s, e = two_sum(a, b)
            sums.append(s)
            lost = e if lost is None else lost + e
        rows = sums
    return rows[0], lost


def coefficients(norms, crosses):
    nu = []
    for k in range(STEPS):
        if k == 0:
            nu += [norms[0], crosses[0]]
        elif k < STEPS - 1:
            nu += [pair_sub(norms[k], norms[k - 1]), pair_sub(crosses[k], crosses[k - 1])]
        else:
            twice = pair_add(crosses[k - 1], crosses[k - 1])
            nu += [pair_sub(norms[k], norms[k - 1]), pair_sub(crosses[k], twice)]
    older, old = {}, dict(enumerate(nu))
    ratio = pair_div(old[1], old[0])
    diag, square = [ratio], []
    for k in range(1, STEPS):
        new = {}
        for l in range(k, 2 * STEPS - k):
            p, e = two_prod(diag[-1][0], old[l][0])
            e = e + (diag[-1][0] * old[l][1] + diag[-1][1] * old[l][0])
            sides, lost = two_sum(old[l + 1][0], old[l - 1][0])
            lost = lost + (old[l + 1][1] + old[l - 1][1])
            term, d = two_sum(sides, -p)
            lost = (lost - e) + d
            if k > 1:
                p, e = two_prod(square[-1][0], older[l][0])
                e = e + (square[-1][0] * older[l][1] + square[-1][1] * older[l][0])
                term, d = two_sum(term, -p)
                lost = (lost - e) + d
            term = fast_two_sum(term, lost)
            new[l] = term
        square.append(pair_div(new[k], old[k - 1]))
        next_ratio = pair_div(new[k + 1], new[k])
        diag.append(pair_sub(next_ratio, ratio))
        ratio = next_ratio
        older, old = old, new
    return diag, square


def scaling(en_ref):
    energies = [en_ref[i] for i in range(en_ref.shape[0])]
    shift = sum(energies[1:], energies[0]) * (1.0 / len(energies))
    spread = sum((e - shift) * (e - shift) for e in energies) * (1.0 / len(energies))
    return energies, shift, spread + 6.0


def inverse_width(square, nx):
    return 1.0 / jnp.sqrt(jnp.full((1, nx), square, jnp.float32))


def iterate(
    n,
    group,
    sv_ref,
    lev_ref,
    en_ref,
    row_ref,
    basis,
    below,
    above,
    onsite,
    levels,
    stats,
    row_a,
    row_b,
    near,
    far,
    load_sem,
    en_smem,
    met,
    up_send,
    up_recv,
    down_send,
    down_recv,
    near_send,
    near_recv,
    far_send,
    far_recv,
):
    ny, nx = onsite.shape
    rows = ny // CHUNKS
    block_rows = min(BLOCK, rows // 2)
    groups = n // group
    me = lax.axis_index("slab")
    up = lax.rem(me + 1, n)
    down = lax.rem(me + n - 1, n)
    mine = lax.rem(me, group)
    team = me // group

    def ring(d, size):
        return min(d, size - d)

    near_peers = []
    for d in sorted(range(1, group), key=lambda d: -ring(d, group)):
        place = lax.rem(mine + d, group)
        near_peers.append((place, team * group + place))
    long = min(8, groups)
    wide = groups // long
    far_peers = []
    steps = [(a, b) for a in range(wide) for b in range(long) if (a, b) != (0, 0)]
    for a, b in sorted(steps, key=lambda ab: -ring(ab[0], wide) - ring(ab[1], long)):
        place = lax.rem(team // long + a, wide) * long + lax.rem(team + b, long)
        far_peers.append((place, place * group + mine))

    def tell(sem, device):
        pl.semaphore_signal(sem, inc=1, device_id=(device,), device_id_type=MESH)

    barrier = pltpu.get_barrier_semaphore()
    tell(barrier, up)
    tell(barrier, down)

    def load(v, c):
        part = pl.ds(c * rows, rows)
        return pltpu.make_async_copy(
            sv_ref.at[v, 0, part], basis.at[1, v, part], load_sem.at[v * CHUNKS + c]
        )

    load_levels = pltpu.make_async_copy(lev_ref.at[0], levels, load_sem.at[2 * CHUNKS])
    for v in range(2):
        for c in range(CHUNKS):
            load(v, c).start()
    load_levels.start()
    load_energies = pltpu.make_async_copy(en_ref, en_smem, load_sem.at[2 * CHUNKS + 1])
    load_energies.start()

    pl.semaphore_wait(barrier, 2)

    rounds = n.bit_length() - 2

    def hear(r):
        pl.semaphore_wait(met.at[r - 1], 2)

    def say(r, distance):
        tell(met.at[r - 1], lax.rem(me + distance, n))
        tell(met.at[r - 1], lax.rem(me + n - distance, n))

    def halo(k, v, c, upward, half=False):
        part = pl.ds(c * rows, rows)
        if half:
            part = pl.ds(c * rows + (0 if upward else rows // 2), rows // 2)
        landing, send, recv, device = (
            (below, up_send, up_recv, up) if upward else (above, down_send, down_recv, down)
        )
        return pltpu.make_async_remote_copy(
            src_ref=basis.at[k + 1, v, part],
            dst_ref=landing.at[k, v, part],
            send_sem=send.at[k, v, c],
            recv_sem=recv.at[k, v, c],
            device_id=(device,),
            device_id_type=MESH,
        )

    for v in range(2):
        for c in range(CHUNKS):
            load(v, c).wait()
            halo(0, v, c, True).start()
            halo(0, v, c, False).start()

    load_energies.wait()
    energies, shift, square = scaling(en_smem)
    inv_row = inverse_width(square, nx)

    load_levels.wait()

    def fold(x):
        parts = [x[i : i + 8] for i in range(0, x.shape[0], 8)]
        while len(parts) > 1:
            parts = [a + b for a, b in zip(parts[::2], parts[1::2])]
        return parts[0]

    def place_onsite(b, carry):
        part = pl.ds(pl.multiple_of(b * block_rows, block_rows), block_rows)
        ids = levels[part, :]
        value = jnp.full((block_rows, nx), energies[0], jnp.float32)
        for i in range(1, len(energies)):
            value = jnp.where(ids == i, energies[i], value)
        onsite[part, :] = (value - shift) * inv_row
        out = []
        for v in range(2):
            basis[0, v, part, :] = jnp.zeros((block_rows, nx), jnp.float32)
            here = basis[1, v, part, :]
            h, e = two_sum(carry[v][0], fold(here * here))
            out.append((h, carry[v][1] + e))
        return tuple(out)

    def squeeze(total):
        h, l = total
        h, e = two_sum(h[:, :128], h[:, 128:])
        return h, (l[:, :128] + l[:, 128:]) + e

    zero_rows = jnp.zeros((8, nx), jnp.float32)
    none = (zero_rows, zero_rows)
    first_norms = lax.fori_loop(0, ny // block_rows, place_onsite, (none, none))
    for v in range(2):
        stats[4 * STEPS - 4 + v, 0], stats[4 * STEPS - 4 + v, 1] = squeeze(first_norms[v])

    def sweep(k, v, first, count, totals, landed=None):
        def block(b, carry):
            start = pl.multiple_of(first + b * block_rows, block_rows)
            part = pl.ds(start, block_rows)
            before = pl.ds(pl.multiple_of(lax.rem(start + (ny - 8), ny), 8), 8)
            after = pl.ds(pl.multiple_of(lax.rem(start + block_rows, ny), 8), 8)
            here = basis[k + 1, v, part, :]
            tall = jnp.concatenate(
                [basis[k + 1, v, before, :], here, basis[k + 1, v, after, :]], axis=0
            )
            height = block_rows + 16
            beside = pltpu.roll(tall, 1, 0)[8 : 8 + block_rows]
            beside = beside + pltpu.roll(tall, height - 1, 0)[8 : 8 + block_rows]
            beside = beside + (pltpu.roll(here, 1, 1) + pltpu.roll(here, nx - 1, 1))
            if landed is not None:
                one = landed[k, v, part, :]
                beside = beside + (one + one)
            else:
                beside = beside + (below[k, v, part, :] + above[k, v, part, :])
            new = onsite[part, :] * here - inv_row * beside
            out = []
            if landed is None:
                new = new - basis[k, v, part, :]
                basis[k + 2, v, part, :] = new
                out.append(new * new)
            out.append(new * here)
            added = []
            for (h, l), x in zip(carry, out):
                h, e = two_sum(h, fold(x))
                added.append((h, l + e))
            return tuple(added)

        return lax.fori_loop(0, count // block_rows, block, totals)

    sub = lax.broadcasted_iota(jnp.int32, (8, 128), 0)
    lane = lax.broadcasted_iota(jnp.int32, (8, 128), 1)

    def lane_sums(items):
        high = jnp.zeros((8, 128), jnp.float32)
        low = jnp.zeros((8, 128), jnp.float32)
        target = jnp.full((8, 128), 1000, jnp.int32)
        for q, (h, l, place) in enumerate(items):
            for shift_by in (4, 2, 1):
                h, e = two_sum(h, pltpu.roll(h, shift_by, 0))
                l = l + pltpu.roll(l, shift_by, 0) + e
            high = jnp.where(sub == q, h, high)
            low = jnp.where(sub == q, l, low)
            target = jnp.where(sub == q, place, target)
        for shift_by in (64, 32, 16, 8, 4, 2, 1):
            high, e = two_sum(high, pltpu.roll(high, shift_by, 1))
            low = low + pltpu.roll(low, shift_by, 1) + e
        return jnp.where(lane == target, high, 0.0) + jnp.where(
            lane == target + 16, low, 0.0
        )

    def step(k, final_sends=False):
        for v in range(2):
            totals = (none, none)
            for c in range(CHUNKS):
                halo(k, v, c, True).wait_recv()
                halo(k, v, c, False).wait_recv()
                totals = sweep(k, v, c * rows, rows, totals)
                halo(k + 1, v, c, True, final_sends).start()
                halo(k + 1, v, c, False, final_sends).start()
            for q in range(2):
                stats[4 * k + 2 * v + q, 0], stats[4 * k + 2 * v + q, 1] = squeeze(totals[q])

    def last_step():
        k = STEPS - 1
        ends = []
        for v in range(2):
            totals = (none,)
            for c in range(CHUNKS):
                if v == 1 and c == CHUNKS - 1:
                    places = [64 * (i % 4 // 2) + (8 + i // 4 if i % 2 else 1 + i // 4) for i in range(4 * k)]
                    places += [0, 64]
                    packed = jnp.zeros((8, 128), jnp.float32)
                    for i in range(0, len(places), 8):
                        packed = packed + lane_sums(
                            [(stats[j, 0], stats[j, 1], places[j]) for j in range(i, min(i + 8, len(places)))]
                        )
                halo(k, v, c, True, True).wait_recv()
                halo(k, v, c, False, True).wait_recv()
                totals = sweep(k, v, c * rows, rows // 2, totals, below)
                totals = sweep(k, v, c * rows + rows // 2, rows // 2, totals, above)
            ends.append(squeeze(totals[0]))
        return packed + lane_sums([(h, l, 64 * v + 8 + k) for v, (h, l) in enumerate(ends)])

    say(1, 1)
    step(0)

    def middle(k, distance):
        @pl.when(k <= rounds)
        def _():
            hear(k)

        @pl.when(k < rounds)
        def _():
            say(k + 1, distance)

        step(k)
        return distance * 2

    lax.fori_loop(1, STEPS - 2, middle, 2)
    for k in (STEPS - 2, STEPS - 1):
        if k <= rounds:
            hear(k)
        if k < rounds:
            say(k + 1, 2**k)
        if k == STEPS - 2:
            step(k, final_sends=True)
    packed = last_step()
    if rounds == STEPS:
        hear(rounds)

    for shift_by in (4, 2, 1):
        packed = packed + pltpu.roll(packed, shift_by, 0)

    row_lane = lax.broadcasted_iota(jnp.int32, (1, 128), 1)
    is_high = lax.rem(row_lane, 64) < 16

    def drain(k, _):
        for v in range(2):
            for c in range(CHUNKS):
                halo(k, v, c, True).wait_send()
                halo(k, v, c, False).wait_send()
        return None

    def drain_all():
        lax.fori_loop(0, STEPS - 1, drain, None)
        for v in range(2):
            for c in range(CHUNKS):
                halo(STEPS - 1, v, c, True, True).wait_send()
                halo(STEPS - 1, v, c, False, True).wait_send()

    def exchange(row, staging, slots, place, peers, send, recv, meanwhile):
        def copy(i, slot):
            return pltpu.make_async_remote_copy(
                src_ref=staging,
                dst_ref=slots.at[slot],
                send_sem=send.at[i],
                recv_sem=recv.at[slot],
                device_id=(peers[i][1],),
                device_id_type=MESH,
            )

        staging[...] = row
        slots[place] = row
        for i in range(len(peers)):
            copy(i, place).start()
        meanwhile()
        for i in reversed(range(len(peers))):
            copy(i, peers[i][0]).wait_recv()
        total, lost = tree_rows([slots[i] for i in range(len(peers) + 1)])
        return jnp.where(is_high, total, total + pltpu.roll(lost, 16, 1)), [
            copy(i, place) for i in range(len(peers))
        ]

    row, sent = exchange(packed[0:1], row_a, near, mine, near_peers, near_send, near_recv, drain_all)

    def drain_near():
        for copy in sent:
            copy.wait_send()

    row, more = exchange(
        row, row_b, far, team, far_peers, far_send, far_recv, drain_near
    )
    row = jnp.where(row_lane == 40, shift, row)
    row = jnp.where(row_lane == 41, inv_row[:, :128], row)
    row_ref[...] = row
    for copy in more:
        copy.wait_send()


def combine(
    row_ref,
    basis,
    field_ref,
    diag_ref,
    off_ref,
    mom_ref,
    field,
    diag_out,
    off_out,
    mom_out,
    table,
    out_sem,
    small_sem,
):
    ny, nx = field.shape[1:]

    row = row_ref[...]
    row_lane = lax.broadcasted_iota(jnp.int32, (1, 128), 1)
    shift = jnp.sum(jnp.where(row_lane == 40, row, 0.0), axis=1, keepdims=True)
    inv_row = jnp.sum(jnp.where(row_lane == 41, row, 0.0), axis=1, keepdims=True)
    tall_row = lax.broadcasted_iota(jnp.int32, (32, 128), 0)
    tall_lane = lax.broadcasted_iota(jnp.int32, (32, 128), 1)
    spread_row = jnp.broadcast_to(row, (32, 128))
    first = jnp.sum(jnp.where(tall_lane == tall_row, spread_row, 0.0), axis=1, keepdims=True)
    second = jnp.sum(
        jnp.where(tall_lane == tall_row + 64, spread_row, 0.0), axis=1, keepdims=True
    )
    table[...] = jnp.where(tall_lane < 64, first, second)

    norms = [(table[k : k + 1, :], table[16 + k : 17 + k, :]) for k in range(STEPS)]
    crosses = [(table[8 + k : 9 + k, :], table[24 + k : 25 + k, :]) for k in range(STEPS)]
    diag, square = coefficients(norms, crosses)

    width = jnp.broadcast_to(1.0 / inv_row, (1, 128))
    alphas = [shift + width * a[0] for a in diag]
    betas = [width * jnp.sqrt(b[0]) for b in square]
    zero = jnp.zeros((1, 128), jnp.float32)
    left = [zero] + betas
    right = betas + [zero]
    emin = functools.reduce(jnp.minimum, [a - p - q for a, p, q in zip(alphas, left, right)])
    emax = functools.reduce(jnp.maximum, [a + p + q for a, p, q in zip(alphas, left, right)])
    center = (emax + emin) * 0.5
    inv_half = 1.0 / (0.55 * (emax - emin))
    slope = width * inv_half
    offset = (shift - center) * inv_half

    def apply(poly):
        around = [zero] + poly + [zero]
        out = []
        for k in range(len(poly) + 1):
            value = slope * around[k] if k else None
            if k < len(poly):
                value = offset * poly[k] if value is None else value + offset * poly[k]
            if k + 2 < len(around) - 1:
                value = value + slope * around[k + 2]
            out.append(value)
        return out

    t0 = [zero + 1.0]
    t1 = apply(t0)
    t2 = [2.0 * q for q in apply(t1)]
    t2[0] = t2[0] - 1.0
    t3 = [2.0 * q for q in apply(t2)]
    t3 = [q - t1[k] if k < 2 else q for k, q in enumerate(t3)]

    inv_norm = 1.0 / norms[0][0]
    size = [q[0] * inv_norm for q in norms[:4]]
    cross = [q[0] * inv_norm for q in crosses[:3]]
    skip = pair_sub(norms[1], norms[0])[0] * inv_norm
    skip_next = pair_sub(norms[2], norms[0])[0] * inv_norm
    skip_two = pair_sub(crosses[1], crosses[0])[0] * inv_norm
    gram = [
        [zero + 1.0, cross[0], skip, skip_two],
        [cross[0], size[1], cross[1], skip_next],
        [skip, cross[1], size[2], cross[2]],
        [skip_two, skip_next, cross[2], size[3]],
    ]

    def inner(p, q):
        return sum(
            a * sum(b * gram[i][j] for j, b in enumerate(q)) for i, a in enumerate(p)
        )

    d01 = inner(t0, t1)
    moments = [
        d01,
        inner(t0, t2),
        inner(t0, t3),
        2.0 * inner(t2, t2) - 1.0,
        2.0 * inner(t3, t2) - d01,
        2.0 * inner(t3, t3) - 1.0,
    ]

    def emit(ref, values):
        packed = zero
        for k, value in enumerate(values):
            packed = jnp.where(lax.rem(row_lane, 64) == k, value, packed)
        ref[0:1, :] = packed[:, : len(values)]
        ref[1:2, :] = pltpu.roll(packed, 64, 1)[:, : len(values)]

    small = []
    for k, (stage, ref, values) in enumerate(
        [(diag_out, diag_ref, alphas), (off_out, off_ref, betas), (mom_out, mom_ref, moments)]
    ):
        emit(stage, values)
        small.append(pltpu.make_async_copy(stage, ref, small_sem.at[k]))

    half = ny // 4

    def store(v, i):
        part = pl.ds(i * half, half)
        return pltpu.make_async_copy(
            field.at[v, part], field_ref.at[v, 0, part], out_sem.at[v, i]
        )

    for v in range(2):
        own = row_lane < 64 if v == 0 else row_lane >= 64
        scale = [jnp.where(own, q, pltpu.roll(q, 64, 1)) for q in t3]
        scale = [jnp.concatenate([q, q], axis=1) for q in scale]
        for i in range(4):

            def finish(b, _):
                part = pl.ds(pl.multiple_of(i * half + b * BLOCK, BLOCK), BLOCK)
                value = scale[0] * basis[1, v, part, :] + scale[1] * basis[2, v, part, :]
                value = value + scale[2] * basis[3, v, part, :]
                field[v, part, :] = value + scale[3] * basis[4, v, part, :]
                return None

            lax.fori_loop(0, half // BLOCK, finish, None)
            store(v, i).start()
        if v == 0:
            for copy in small:
                copy.start()

    for v in range(2):
        for i in range(4):
            store(v, i).wait()
    for copy in small:
        copy.wait()


def solution(mesh):
    n = mesh.shape["slab"]
    group = 16 if n >= 128 else 4

    def shards(start_vectors, levels, energies):
        vecs, _, ny, nx = start_vectors.shape
        f32 = jnp.float32
        dma = pltpu.SemaphoreType.DMA
        vmem = pl.BlockSpec(memory_space=pltpu.VMEM)
        hbm = pl.BlockSpec(memory_space=pltpu.HBM)
        halo_sem = dma((STEPS, vecs, CHUNKS))
        groups = n // group
        row, basis = pl.pallas_call(
            functools.partial(iterate, n, group),
            out_shape=(
                pltpu.VMEM((1, 128), f32),
                pltpu.VMEM((STEPS + 1, vecs, ny, nx), f32),
            ),
            in_specs=[hbm, hbm, hbm],
            out_specs=(vmem, vmem),
            scratch_shapes=[
                pltpu.VMEM((STEPS, vecs, ny, nx), f32),
                pltpu.VMEM((STEPS, vecs, ny, nx), f32),
                pltpu.VMEM((ny, nx), f32),
                pltpu.VMEM((ny, nx), jnp.int32),
                pltpu.VMEM((4 * STEPS - 2, 2, 8, 128), f32),
                pltpu.VMEM((1, 128), f32),
                pltpu.VMEM((1, 128), f32),
                pltpu.VMEM((group, 1, 128), f32),
                pltpu.VMEM((groups, 1, 128), f32),
                dma((2 * CHUNKS + 2,)),
                pltpu.SMEM(energies.shape, f32),
                pltpu.SemaphoreType.REGULAR((STEPS,)),
                halo_sem,
                halo_sem,
                halo_sem,
                halo_sem,
                dma((group,)),
                dma((group,)),
                dma((groups,)),
                dma((groups,)),
            ],
            compiler_params=pltpu.CompilerParams(
                collective_id=0, has_side_effects=True, vmem_limit_bytes=62_000_000
            ),
        )(start_vectors, levels, energies)
        return pl.pallas_call(
            combine,
            out_shape=(
                jax.ShapeDtypeStruct(start_vectors.shape, f32),
                jax.ShapeDtypeStruct((vecs, STEPS), f32),
                jax.ShapeDtypeStruct((vecs, STEPS - 1), f32),
                jax.ShapeDtypeStruct((vecs, 6), f32),
            ),
            in_specs=[vmem, vmem],
            out_specs=(hbm, hbm, hbm, hbm),
            scratch_shapes=[
                pltpu.VMEM((vecs, ny, nx), f32),
                pltpu.VMEM((vecs, STEPS), f32),
                pltpu.VMEM((vecs, STEPS - 1), f32),
                pltpu.VMEM((vecs, 6), f32),
                pltpu.VMEM((32, 128), f32),
                dma((vecs, 4)),
                dma((3,)),
            ],
            compiler_params=pltpu.CompilerParams(vmem_limit_bytes=8 * 2**20),
        )(row, basis)

    return jax.shard_map(
        shards,
        mesh=mesh,
        in_specs=(P(None, "slab", None, None), P("slab", None, None), P()),
        out_specs=(P(None, "slab", None, None), P(), P(), P()),
        check_vma=False,
    )
```

```python
import functools

import jax
import jax.numpy as jnp
from jax import lax
from jax.experimental import pallas as pl
from jax.experimental.pallas import tpu as pltpu
from jax.sharding import PartitionSpec as P

STEPS = 8
CHUNKS = 4
BLOCK = 32
MESH = pl.DeviceIdType.MESH


def two_sum(a, b):
    s = a + b
    t = s - a
    return s, (a - (s - t)) + (b - t)


def fast_two_sum(a, b):
    s = a + b
    return s, b - (s - a)


def split(a):
    t = a * 4097.0
    high = t - (t - a)
    return high, a - high


def two_prod(a, b):
    p = a * b
    ah, al = split(a)
    bh, bl = split(b)
    return p, ((ah * bh - p) + ah * bl + al * bh) + al * bl


def pair_add(a, b):
    s, e = two_sum(a[0], b[0])
    return fast_two_sum(s, e + (a[1] + b[1]))


def pair_neg(a):
    return -a[0], -a[1]


def pair_sub(a, b):
    return pair_add(a, pair_neg(b))


def pair_mul(a, b):
    p, e = two_prod(a[0], b[0])
    return fast_two_sum(p, e + (a[0] * b[1] + a[1] * b[0]))


def pair_div(a, b):
    inv = 1.0 / b[0]
    first = a[0] * inv
    p, e = two_prod(first, b[0])
    rest = (a[0] - p) - e + a[1] - first * b[1]
    return fast_two_sum(first, rest * inv)


def tree_rows(rows):
    lost = None
    while len(rows) > 1:
        sums = []
        for a, b in zip(rows[::2], rows[1::2]):
            s, e = two_sum(a, b)
            sums.append(s)
            lost = e if lost is None else lost + e
        rows = sums
    return rows[0], lost


def coefficients(norms, crosses):
    nu = []
    for k in range(STEPS):
        if k == 0:
            nu += [norms[0], crosses[0]]
        elif k < STEPS - 1:
            nu += [pair_sub(norms[k], norms[k - 1]), pair_sub(crosses[k], crosses[k - 1])]
        else:
            twice = pair_add(crosses[k - 1], crosses[k - 1])
            nu += [pair_sub(norms[k], norms[k - 1]), pair_sub(crosses[k], twice)]
    older, old = {}, dict(enumerate(nu))
    ratio = pair_div(old[1], old[0])
    diag, square = [ratio], []
    for k in range(1, STEPS):
        new = {}
        for l in range(k, 2 * STEPS - k):
            p, e = two_prod(diag[-1][0], old[l][0])
            e = e + (diag[-1][0] * old[l][1] + diag[-1][1] * old[l][0])
            sides, lost = two_sum(old[l + 1][0], old[l - 1][0])
            lost = lost + (old[l + 1][1] + old[l - 1][1])
            term, d = two_sum(sides, -p)
            lost = (lost - e) + d
            if k > 1:
                p, e = two_prod(square[-1][0], older[l][0])
                e = e + (square[-1][0] * older[l][1] + square[-1][1] * older[l][0])
                term, d = two_sum(term, -p)
                lost = (lost - e) + d
            term = fast_two_sum(term, lost)
            new[l] = term
        square.append(pair_div(new[k], old[k - 1]))
        next_ratio = pair_div(new[k + 1], new[k])
        diag.append(pair_sub(next_ratio, ratio))
        ratio = next_ratio
        older, old = old, new
    return diag, square


def scaling(en_ref):
    energies = [en_ref[i] for i in range(en_ref.shape[0])]
    shift = sum(energies[1:], energies[0]) * (1.0 / len(energies))
    spread = sum((e - shift) * (e - shift) for e in energies) * (1.0 / len(energies))
    return energies, shift, spread + 9.0


def inverse_width(square, nx):
    return 1.0 / jnp.sqrt(jnp.full((1, nx), square, jnp.float32))


def iterate(
    n,
    group,
    sv_ref,
    lev_ref,
    en_ref,
    row_ref,
    basis,
    below,
    above,
    onsite,
    levels,
    stats,
    row_a,
    row_b,
    near,
    far,
    load_sem,
    en_smem,
    met,
    up_send,
    up_recv,
    down_send,
    down_recv,
    near_send,
    near_recv,
    far_send,
    far_recv,
):
    ny, nx = onsite.shape
    rows = ny // CHUNKS
    block_rows = min(BLOCK, rows // 2)
    groups = n // group
    me = lax.axis_index("slab")
    up = lax.rem(me + 1, n)
    down = lax.rem(me + n - 1, n)
    mine = lax.rem(me, group)
    team = me // group

    def ring(d, size):
        return min(d, size - d)

    near_peers = []
    for d in sorted(range(1, group), key=lambda d: -ring(d, group)):
        place = lax.rem(mine + d, group)
        near_peers.append((place, team * group + place))
    long = min(8, groups)
    wide = groups // long
    far_peers = []
    steps = [(a, b) for a in range(wide) for b in range(long) if (a, b) != (0, 0)]
    for a, b in sorted(steps, key=lambda ab: -ring(ab[0], wide) - ring(ab[1], long)):
        place = lax.rem(team // long + a, wide) * long + lax.rem(team + b, long)
        far_peers.append((place, place * group + mine))

    def tell(sem, device):
        pl.semaphore_signal(sem, inc=1, device_id=(device,), device_id_type=MESH)

    barrier = pltpu.get_barrier_semaphore()
    tell(barrier, up)
    tell(barrier, down)

    def load(v, c):
        part = pl.ds(c * rows, rows)
        return pltpu.make_async_copy(
            sv_ref.at[v, 0, part], basis.at[1, v, part], load_sem.at[v * CHUNKS + c]
        )

    load_levels = pltpu.make_async_copy(lev_ref.at[0], levels, load_sem.at[2 * CHUNKS])
    for v in range(2):
        for c in range(CHUNKS):
            load(v, c).start()
    load_levels.start()
    load_energies = pltpu.make_async_copy(en_ref, en_smem, load_sem.at[2 * CHUNKS + 1])
    load_energies.start()

    pl.semaphore_wait(barrier, 2)

    rounds = n.bit_length() - 2

    def hear(r):
        pl.semaphore_wait(met.at[r - 1], 2)

    def say(r, distance):
        tell(met.at[r - 1], lax.rem(me + distance, n))
        tell(met.at[r - 1], lax.rem(me + n - distance, n))

    def halo(k, v, c, upward, half=False):
        part = pl.ds(c * rows, rows)
        if half:
            part = pl.ds(c * rows + (0 if upward else rows // 2), rows // 2)
        landing, send, recv, device = (
            (below, up_send, up_recv, up) if upward else (above, down_send, down_recv, down)
        )
        return pltpu.make_async_remote_copy(
            src_ref=basis.at[k + 1, v, part],
            dst_ref=landing.at[k, v, part],
            send_sem=send.at[k, v, c],
            recv_sem=recv.at[k, v, c],
            device_id=(device,),
            device_id_type=MESH,
        )

    for v in range(2):
        for c in range(CHUNKS):
            load(v, c).wait()
            halo(0, v, c, True).start()
            halo(0, v, c, False).start()

    load_energies.wait()
    energies, shift, square = scaling(en_smem)
    inv_row = inverse_width(square, nx)

    load_levels.wait()

    def fold(x):
        parts = [x[i : i + 8] for i in range(0, x.shape[0], 8)]
        while len(parts) > 1:
            parts = [a + b for a, b in zip(parts[::2], parts[1::2])]
        return parts[0]

    def place_onsite(b, carry):
        part = pl.ds(pl.multiple_of(b * block_rows, block_rows), block_rows)
        ids = levels[part, :]
        value = jnp.full((block_rows, nx), energies[0], jnp.float32)
        for i in range(1, len(energies)):
            value = jnp.where(ids == i, energies[i], value)
        onsite[part, :] = (value - shift) * inv_row
        out = []
        for v in range(2):
            basis[0, v, part, :] = jnp.zeros((block_rows, nx), jnp.float32)
            here = basis[1, v, part, :]
            h, e = two_sum(carry[v][0], fold(here * here))
            out.append((h, carry[v][1] + e))
        return tuple(out)

    def squeeze(total):
        h, l = total
        h, e = two_sum(h[:, :128], h[:, 128:])
        return h, (l[:, :128] + l[:, 128:]) + e

    zero_rows = jnp.zeros((8, nx), jnp.float32)
    none = (zero_rows, zero_rows)
    first_norms = lax.fori_loop(0, ny // block_rows, place_onsite, (none, none))
    for v in range(2):
        stats[4 * STEPS - 4 + v, 0], stats[4 * STEPS - 4 + v, 1] = squeeze(first_norms[v])

    def sweep(k, v, first, count, totals, landed=None):
        def block(b, carry):
            start = pl.multiple_of(first + b * block_rows, block_rows)
            part = pl.ds(start, block_rows)
            before = pl.ds(pl.multiple_of(lax.rem(start + (ny - 8), ny), 8), 8)
            after = pl.ds(pl.multiple_of(lax.rem(start + block_rows, ny), 8), 8)
            here = basis[k + 1, v, part, :]
            tall = jnp.concatenate(
                [basis[k + 1, v, before, :], here, basis[k + 1, v, after, :]], axis=0
            )
            height = block_rows + 16
            beside = pltpu.roll(tall, 1, 0)[8 : 8 + block_rows]
            beside = beside + pltpu.roll(tall, height - 1, 0)[8 : 8 + block_rows]
            beside = beside + (pltpu.roll(here, 1, 1) + pltpu.roll(here, nx - 1, 1))
            if landed is not None:
                one = landed[k, v, part, :]
                beside = beside + (one + one)
            else:
                beside = beside + (below[k, v, part, :] + above[k, v, part, :])
            new = onsite[part, :] * here - inv_row * beside
            out = []
            if landed is None:
                new = new - basis[k, v, part, :]
                basis[k + 2, v, part, :] = new
                out.append(new * new)
            out.append(new * here)
            added = []
            for (h, l), x in zip(carry, out):
                h, e = two_sum(h, fold(x))
                added.append((h, l + e))
            return tuple(added)

        return lax.fori_loop(0, count // block_rows, block, totals)

    sub = lax.broadcasted_iota(jnp.int32, (8, 128), 0)
    lane = lax.broadcasted_iota(jnp.int32, (8, 128), 1)

    def lane_sums(items):
        high = jnp.zeros((8, 128), jnp.float32)
        low = jnp.zeros((8, 128), jnp.float32)
        target = jnp.full((8, 128), 1000, jnp.int32)
        for q, (h, l, place) in enumerate(items):
            for shift_by in (4, 2, 1):
                h, e = two_sum(h, pltpu.roll(h, shift_by, 0))
                l = l + pltpu.roll(l, shift_by, 0) + e
            high = jnp.where(sub == q, h, high)
            low = jnp.where(sub == q, l, low)
            target = jnp.where(sub == q, place, target)
        for shift_by in (64, 32, 16, 8, 4, 2, 1):
            high, e = two_sum(high, pltpu.roll(high, shift_by, 1))
            low = low + pltpu.roll(low, shift_by, 1) + e
        return jnp.where(lane == target, high, 0.0) + jnp.where(
            lane == target + 16, low, 0.0
        )

    def step(k, final_sends=False):
        for v in range(2):
            totals = (none, none)
            for c in range(CHUNKS):
                halo(k, v, c, True).wait_recv()
                halo(k, v, c, False).wait_recv()
                totals = sweep(k, v, c * rows, rows, totals)
                halo(k + 1, v, c, True, final_sends).start()
                halo(k + 1, v, c, False, final_sends).start()
            for q in range(2):
                stats[4 * k + 2 * v + q, 0], stats[4 * k + 2 * v + q, 1] = squeeze(totals[q])

    def last_step():
        k = STEPS - 1
        ends = []
        for v in range(2):
            totals = (none,)
            for c in range(CHUNKS):
                if v == 1 and c == CHUNKS - 1:
                    places = [64 * (i % 4 // 2) + (8 + i // 4 if i % 2 else 1 + i // 4) for i in range(4 * k)]
                    places += [0, 64]
                    packed = jnp.zeros((8, 128), jnp.float32)
                    for i in range(0, len(places), 8):
                        packed = packed + lane_sums(
                            [(stats[j, 0], stats[j, 1], places[j]) for j in range(i, min(i + 8, len(places)))]
                        )
                halo(k, v, c, True, True).wait_recv()
                halo(k, v, c, False, True).wait_recv()
                totals = sweep(k, v, c * rows, rows // 2, totals, below)
                totals = sweep(k, v, c * rows + rows // 2, rows // 2, totals, above)
            ends.append(squeeze(totals[0]))
        return packed + lane_sums([(h, l, 64 * v + 8 + k) for v, (h, l) in enumerate(ends)])

    say(1, 1)
    step(0)

    def middle(k, distance):
        @pl.when(k <= rounds)
        def _():
            hear(k)

        @pl.when(k < rounds)
        def _():
            say(k + 1, distance)

        step(k)
        return distance * 2

    lax.fori_loop(1, STEPS - 2, middle, 2)
    for k in (STEPS - 2, STEPS - 1):
        if k <= rounds:
            hear(k)
        if k < rounds:
            say(k + 1, 2**k)
        if k == STEPS - 2:
            step(k, final_sends=True)
    packed = last_step()
    if rounds == STEPS:
        hear(rounds)

    for shift_by in (4, 2, 1):
        packed = packed + pltpu.roll(packed, shift_by, 0)

    row_lane = lax.broadcasted_iota(jnp.int32, (1, 128), 1)
    is_high = lax.rem(row_lane, 64) < 16

    def drain(k, _):
        for v in range(2):
            for c in range(CHUNKS):
                halo(k, v, c, True).wait_send()
                halo(k, v, c, False).wait_send()
        return None

    def drain_all():
        lax.fori_loop(0, STEPS - 1, drain, None)
        for v in range(2):
            for c in range(CHUNKS):
                halo(STEPS - 1, v, c, True, True).wait_send()
                halo(STEPS - 1, v, c, False, True).wait_send()

    def exchange(row, staging, slots, place, peers, send, recv, meanwhile):
        def copy(i, slot):
            return pltpu.make_async_remote_copy(
                src_ref=staging,
                dst_ref=slots.at[slot],
                send_sem=send.at[i],
                recv_sem=recv.at[slot],
                device_id=(peers[i][1],),
                device_id_type=MESH,
            )

        staging[...] = row
        slots[place] = row
        for i in range(len(peers)):
            copy(i, place).start()
        meanwhile()
        for i in reversed(range(len(peers))):
            copy(i, peers[i][0]).wait_recv()
        total, lost = tree_rows([slots[i] for i in range(len(peers) + 1)])
        return jnp.where(is_high, total, total + pltpu.roll(lost, 16, 1)), [
            copy(i, place) for i in range(len(peers))
        ]

    row, sent = exchange(
        packed[0:1], row_b, far, team, far_peers, far_send, far_recv, drain_all
    )

    def drain_first():
        for copy in sent:
            copy.wait_send()

    row, more = exchange(
        row, row_a, near, mine, near_peers, near_send, near_recv, drain_first
    )
    row = jnp.where(row_lane == 40, shift, row)
    row = jnp.where(row_lane == 41, inv_row[:, :128], row)
    row_ref[...] = row
    for copy in more:
        copy.wait_send()


def combine(
    row_ref,
    basis,
    field_ref,
    diag_ref,
    off_ref,
    mom_ref,
    field,
    diag_out,
    off_out,
    mom_out,
    table,
    out_sem,
    small_sem,
):
    ny, nx = field.shape[1:]

    row = row_ref[...]
    row_lane = lax.broadcasted_iota(jnp.int32, (1, 128), 1)
    shift = jnp.sum(jnp.where(row_lane == 40, row, 0.0), axis=1, keepdims=True)
    inv_row = jnp.sum(jnp.where(row_lane == 41, row, 0.0), axis=1, keepdims=True)
    tall_row = lax.broadcasted_iota(jnp.int32, (32, 128), 0)
    tall_lane = lax.broadcasted_iota(jnp.int32, (32, 128), 1)
    spread_row = jnp.broadcast_to(row, (32, 128))
    first = jnp.sum(jnp.where(tall_lane == tall_row, spread_row, 0.0), axis=1, keepdims=True)
    second = jnp.sum(
        jnp.where(tall_lane == tall_row + 64, spread_row, 0.0), axis=1, keepdims=True
    )
    table[...] = jnp.where(tall_lane < 64, first, second)

    norms = [(table[k : k + 1, :], table[16 + k : 17 + k, :]) for k in range(STEPS)]
    crosses = [(table[8 + k : 9 + k, :], table[24 + k : 25 + k, :]) for k in range(STEPS)]
    diag, square = coefficients(norms, crosses)

    width = jnp.broadcast_to(1.0 / inv_row, (1, 128))
    alphas = [shift + width * a[0] for a in diag]
    betas = [width * jnp.sqrt(b[0]) for b in square]
    zero = jnp.zeros((1, 128), jnp.float32)
    left = [zero] + betas
    right = betas + [zero]
    emin = functools.reduce(jnp.minimum, [a - p - q for a, p, q in zip(alphas, left, right)])
    emax = functools.reduce(jnp.maximum, [a + p + q for a, p, q in zip(alphas, left, right)])
    center = (emax + emin) * 0.5
    inv_half = 1.0 / (0.55 * (emax - emin))
    slope = width * inv_half
    offset = (shift - center) * inv_half

    def apply(poly):
        around = [zero] + poly + [zero]
        out = []
        for k in range(len(poly) + 1):
            value = slope * around[k] if k else None
            if k < len(poly):
                value = offset * poly[k] if value is None else value + offset * poly[k]
            if k + 2 < len(around) - 1:
                value = value + slope * around[k + 2]
            out.append(value)
        return out

    t0 = [zero + 1.0]
    t1 = apply(t0)
    t2 = [2.0 * q for q in apply(t1)]
    t2[0] = t2[0] - 1.0
    t3 = [2.0 * q for q in apply(t2)]
    t3 = [q - t1[k] if k < 2 else q for k, q in enumerate(t3)]

    inv_norm = 1.0 / norms[0][0]
    size = [q[0] * inv_norm for q in norms[:4]]
    cross = [q[0] * inv_norm for q in crosses[:3]]
    skip = pair_sub(norms[1], norms[0])[0] * inv_norm
    skip_next = pair_sub(norms[2], norms[0])[0] * inv_norm
    skip_two = pair_sub(crosses[1], crosses[0])[0] * inv_norm
    gram = [
        [zero + 1.0, cross[0], skip, skip_two],
        [cross[0], size[1], cross[1], skip_next],
        [skip, cross[1], size[2], cross[2]],
        [skip_two, skip_next, cross[2], size[3]],
    ]

    def inner(p, q):
        return sum(
            a * sum(b * gram[i][j] for j, b in enumerate(q)) for i, a in enumerate(p)
        )

    d01 = inner(t0, t1)
    moments = [
        d01,
        inner(t0, t2),
        inner(t0, t3),
        2.0 * inner(t2, t2) - 1.0,
        2.0 * inner(t3, t2) - d01,
        2.0 * inner(t3, t3) - 1.0,
    ]

    def emit(ref, values):
        packed = zero
        for k, value in enumerate(values):
            packed = jnp.where(lax.rem(row_lane, 64) == k, value, packed)
        ref[0:1, :] = packed[:, : len(values)]
        ref[1:2, :] = pltpu.roll(packed, 64, 1)[:, : len(values)]

    small = []
    for k, (stage, ref, values) in enumerate(
        [(diag_out, diag_ref, alphas), (off_out, off_ref, betas), (mom_out, mom_ref, moments)]
    ):
        emit(stage, values)
        small.append(pltpu.make_async_copy(stage, ref, small_sem.at[k]))

    half = ny // 4

    def store(v, i):
        part = pl.ds(i * half, half)
        return pltpu.make_async_copy(
            field.at[v, part], field_ref.at[v, 0, part], out_sem.at[v, i]
        )

    for v in range(2):
        own = row_lane < 64 if v == 0 else row_lane >= 64
        scale = [jnp.where(own, q, pltpu.roll(q, 64, 1)) for q in t3]
        scale = [jnp.concatenate([q, q], axis=1) for q in scale]
        for i in range(4):

            def finish(b, _):
                part = pl.ds(pl.multiple_of(i * half + b * BLOCK, BLOCK), BLOCK)
                value = scale[0] * basis[1, v, part, :] + scale[1] * basis[2, v, part, :]
                value = value + scale[2] * basis[3, v, part, :]
                field[v, part, :] = value + scale[3] * basis[4, v, part, :]
                return None

            lax.fori_loop(0, half // BLOCK, finish, None)
            store(v, i).start()
        if v == 0:
            for copy in small:
                copy.start()

    for v in range(2):
        for i in range(4):
            store(v, i).wait()
    for copy in small:
        copy.wait()


def solution(mesh):
    n = mesh.shape["slab"]
    group = 16 if n >= 128 else 4

    def shards(start_vectors, levels, energies):
        vecs, _, ny, nx = start_vectors.shape
        f32 = jnp.float32
        dma = pltpu.SemaphoreType.DMA
        vmem = pl.BlockSpec(memory_space=pltpu.VMEM)
        hbm = pl.BlockSpec(memory_space=pltpu.HBM)
        halo_sem = dma((STEPS, vecs, CHUNKS))
        groups = n // group
        row, basis = pl.pallas_call(
            functools.partial(iterate, n, group),
            out_shape=(
                pltpu.VMEM((1, 128), f32),
                pltpu.VMEM((STEPS + 1, vecs, ny, nx), f32),
            ),
            in_specs=[hbm, hbm, hbm],
            out_specs=(vmem, vmem),
            scratch_shapes=[
                pltpu.VMEM((STEPS, vecs, ny, nx), f32),
                pltpu.VMEM((STEPS, vecs, ny, nx), f32),
                pltpu.VMEM((ny, nx), f32),
                pltpu.VMEM((ny, nx), jnp.int32),
                pltpu.VMEM((4 * STEPS - 2, 2, 8, 128), f32),
                pltpu.VMEM((1, 128), f32),
                pltpu.VMEM((1, 128), f32),
                pltpu.VMEM((group, 1, 128), f32),
                pltpu.VMEM((groups, 1, 128), f32),
                dma((2 * CHUNKS + 2,)),
                pltpu.SMEM(energies.shape, f32),
                pltpu.SemaphoreType.REGULAR((STEPS,)),
                halo_sem,
                halo_sem,
                halo_sem,
                halo_sem,
                dma((group,)),
                dma((group,)),
                dma((groups,)),
                dma((groups,)),
            ],
            compiler_params=pltpu.CompilerParams(
                collective_id=0, has_side_effects=True, vmem_limit_bytes=62_000_000
            ),
        )(start_vectors, levels, energies)
        return pl.pallas_call(
            combine,
            out_shape=(
                jax.ShapeDtypeStruct(start_vectors.shape, f32),
                jax.ShapeDtypeStruct((vecs, STEPS), f32),
                jax.ShapeDtypeStruct((vecs, STEPS - 1), f32),
                jax.ShapeDtypeStruct((vecs, 6), f32),
            ),
            in_specs=[vmem, vmem],
            out_specs=(hbm, hbm, hbm, hbm),
            scratch_shapes=[
                pltpu.VMEM((vecs, ny, nx), f32),
                pltpu.VMEM((vecs, STEPS), f32),
                pltpu.VMEM((vecs, STEPS - 1), f32),
                pltpu.VMEM((vecs, 6), f32),
                pltpu.VMEM((32, 128), f32),
                dma((vecs, 4)),
                dma((3,)),
            ],
            compiler_params=pltpu.CompilerParams(vmem_limit_bytes=8 * 2**20),
        )(row, basis)

    return jax.shard_map(
        shards,
        mesh=mesh,
        in_specs=(P(None, "slab", None, None), P("slab", None, None), P()),
        out_specs=(P(None, "slab", None, None), P(), P(), P()),
        check_vma=False,
    )
```

```python
import functools

import jax
import jax.numpy as jnp
from jax import lax
from jax.experimental import pallas as pl
from jax.experimental.pallas import tpu as pltpu
from jax.sharding import PartitionSpec as P

STEPS = 8
CHUNKS = 4
BLOCK = 32
MESH = pl.DeviceIdType.MESH


def two_sum(a, b):
    s = a + b
    t = s - a
    return s, (a - (s - t)) + (b - t)


def fast_two_sum(a, b):
    s = a + b
    return s, b - (s - a)


def split(a):
    t = a * 4097.0
    high = t - (t - a)
    return high, a - high


def two_prod(a, b):
    p = a * b
    ah, al = split(a)
    bh, bl = split(b)
    return p, ((ah * bh - p) + ah * bl + al * bh) + al * bl


def pair_add(a, b):
    s, e = two_sum(a[0], b[0])
    return fast_two_sum(s, e + (a[1] + b[1]))


def pair_neg(a):
    return -a[0], -a[1]


def pair_sub(a, b):
    return pair_add(a, pair_neg(b))


def pair_mul(a, b):
    p, e = two_prod(a[0], b[0])
    return fast_two_sum(p, e + (a[0] * b[1] + a[1] * b[0]))


def pair_div(a, b):
    inv = 1.0 / b[0]
    first = a[0] * inv
    p, e = two_prod(first, b[0])
    rest = (a[0] - p) - e + a[1] - first * b[1]
    return fast_two_sum(first, rest * inv)


def tree_rows(rows):
    lost = None
    while len(rows) > 1:
        sums = []
        for a, b in zip(rows[::2], rows[1::2]):
            s, e = two_sum(a, b)
            sums.append(s)
            lost = e if lost is None else lost + e
        rows = sums
    return rows[0], lost


def coefficients(norms, crosses):
    nu = []
    for k in range(STEPS):
        if k == 0:
            nu += [norms[0], crosses[0]]
        elif k < STEPS - 1:
            nu += [pair_sub(norms[k], norms[k - 1]), pair_sub(crosses[k], crosses[k - 1])]
        else:
            twice = pair_add(crosses[k - 1], crosses[k - 1])
            nu += [pair_sub(norms[k], norms[k - 1]), pair_sub(crosses[k], twice)]
    older, old = {}, dict(enumerate(nu))
    ratio = pair_div(old[1], old[0])
    diag, square = [ratio], []
    for k in range(1, STEPS):
        new = {}
        for l in range(k, 2 * STEPS - k):
            p, e = two_prod(diag[-1][0], old[l][0])
            e = e + (diag[-1][0] * old[l][1] + diag[-1][1] * old[l][0])
            sides, lost = two_sum(old[l + 1][0], old[l - 1][0])
            lost = lost + (old[l + 1][1] + old[l - 1][1])
            term, d = two_sum(sides, -p)
            lost = (lost - e) + d
            if k > 1:
                p, e = two_prod(square[-1][0], older[l][0])
                e = e + (square[-1][0] * older[l][1] + square[-1][1] * older[l][0])
                term, d = two_sum(term, -p)
                lost = (lost - e) + d
            term = fast_two_sum(term, lost)
            new[l] = term
        square.append(pair_div(new[k], old[k - 1]))
        next_ratio = pair_div(new[k + 1], new[k])
        diag.append(pair_sub(next_ratio, ratio))
        ratio = next_ratio
        older, old = old, new
    return diag, square


def scaling(en_ref):
    energies = [en_ref[i] for i in range(en_ref.shape[0])]
    shift = sum(energies[1:], energies[0]) * (1.0 / len(energies))
    spread = sum((e - shift) * (e - shift) for e in energies) * (1.0 / len(energies))
    return energies, shift, spread + 9.0


def inverse_width(square, nx):
    return 1.0 / jnp.sqrt(jnp.full((1, nx), square, jnp.float32))


def iterate(
    n,
    group,
    sv_ref,
    lev_ref,
    en_ref,
    row_ref,
    basis,
    below,
    above,
    onsite,
    levels,
    stats,
    row_a,
    row_b,
    near,
    far,
    load_sem,
    en_smem,
    met,
    up_send,
    up_recv,
    down_send,
    down_recv,
    near_send,
    near_recv,
    far_send,
    far_recv,
):
    ny, nx = onsite.shape
    rows = ny // CHUNKS
    block_rows = min(BLOCK, rows // 2)
    groups = n // group
    me = lax.axis_index("slab")
    up = lax.rem(me + 1, n)
    down = lax.rem(me + n - 1, n)
    mine = lax.rem(me, group)
    team = me // group

    def ring(d, size):
        return min(d, size - d)

    near_peers = []
    for d in sorted(range(1, group), key=lambda d: -ring(d, group)):
        place = lax.rem(mine + d, group)
        near_peers.append((place, team * group + place))
    long = min(8, groups)
    wide = groups // long
    far_peers = []
    steps = [(a, b) for a in range(wide) for b in range(long) if (a, b) != (0, 0)]
    for a, b in sorted(steps, key=lambda ab: -ring(ab[0], wide) - ring(ab[1], long)):
        place = lax.rem(team // long + a, wide) * long + lax.rem(team + b, long)
        far_peers.append((place, place * group + mine))

    def tell(sem, device):
        pl.semaphore_signal(sem, inc=1, device_id=(device,), device_id_type=MESH)

    barrier = pltpu.get_barrier_semaphore()
    tell(barrier, up)
    tell(barrier, down)

    def load(v, c):
        part = pl.ds(c * rows, rows)
        return pltpu.make_async_copy(
            sv_ref.at[v, 0, part], basis.at[1, v, part], load_sem.at[v * CHUNKS + c]
        )

    load_levels = pltpu.make_async_copy(lev_ref.at[0], levels, load_sem.at[2 * CHUNKS])
    for v in range(2):
        for c in range(CHUNKS):
            load(v, c).start()
    load_levels.start()
    load_energies = pltpu.make_async_copy(en_ref, en_smem, load_sem.at[2 * CHUNKS + 1])
    load_energies.start()

    pl.semaphore_wait(barrier, 2)

    rounds = n.bit_length() - 2

    def hear(r):
        pl.semaphore_wait(met.at[r - 1], 2)

    def say(r, distance):
        tell(met.at[r - 1], lax.rem(me + distance, n))
        tell(met.at[r - 1], lax.rem(me + n - distance, n))

    def halo(k, v, c, upward, half=False):
        part = pl.ds(c * rows, rows)
        if half:
            part = pl.ds(c * rows + (0 if upward else rows // 2), rows // 2)
        landing, send, recv, device = (
            (below, up_send, up_recv, up) if upward else (above, down_send, down_recv, down)
        )
        return pltpu.make_async_remote_copy(
            src_ref=basis.at[k + 1, v, part],
            dst_ref=landing.at[k, v, part],
            send_sem=send.at[k, v, c],
            recv_sem=recv.at[k, v, c],
            device_id=(device,),
            device_id_type=MESH,
        )

    for v in range(2):
        for c in range(CHUNKS):
            load(v, c).wait()
            halo(0, v, c, True).start()
            halo(0, v, c, False).start()

    load_energies.wait()
    energies, shift, square = scaling(en_smem)
    inv_row = inverse_width(square, nx)

    load_levels.wait()

    def fold(x):
        parts = [x[i : i + 8] for i in range(0, x.shape[0], 8)]
        while len(parts) > 1:
            parts = [a + b for a, b in zip(parts[::2], parts[1::2])]
        return parts[0]

    def place_onsite(b, carry):
        part = pl.ds(pl.multiple_of(b * block_rows, block_rows), block_rows)
        ids = levels[part, :]
        value = jnp.full((block_rows, nx), energies[0], jnp.float32)
        for i in range(1, len(energies)):
            value = jnp.where(ids == i, energies[i], value)
        onsite[part, :] = (value - shift) * inv_row
        out = []
        for v in range(2):
            basis[0, v, part, :] = jnp.zeros((block_rows, nx), jnp.float32)
            here = basis[1, v, part, :]
            h, e = two_sum(carry[v][0], fold(here * here))
            out.append((h, carry[v][1] + e))
        return tuple(out)

    def squeeze(total):
        h, l = total
        h, e = two_sum(h[:, :128], h[:, 128:])
        return h, (l[:, :128] + l[:, 128:]) + e

    zero_rows = jnp.zeros((8, nx), jnp.float32)
    none = (zero_rows, zero_rows)
    first_norms = lax.fori_loop(0, ny // block_rows, place_onsite, (none, none))
    for v in range(2):
        stats[4 * STEPS - 4 + v, 0], stats[4 * STEPS - 4 + v, 1] = squeeze(first_norms[v])

    def sweep(k, v, first, count, totals, landed=None):
        def block(b, carry):
            start = pl.multiple_of(first + b * block_rows, block_rows)
            part = pl.ds(start, block_rows)
            before = pl.ds(pl.multiple_of(lax.rem(start + (ny - 8), ny), 8), 8)
            after = pl.ds(pl.multiple_of(lax.rem(start + block_rows, ny), 8), 8)
            here = basis[k + 1, v, part, :]
            tall = jnp.concatenate(
                [basis[k + 1, v, before, :], here, basis[k + 1, v, after, :]], axis=0
            )
            height = block_rows + 16
            beside = pltpu.roll(tall, 1, 0)[8 : 8 + block_rows]
            beside = beside + pltpu.roll(tall, height - 1, 0)[8 : 8 + block_rows]
            beside = beside + (pltpu.roll(here, 1, 1) + pltpu.roll(here, nx - 1, 1))
            if landed is not None:
                one = landed[k, v, part, :]
                beside = beside + (one + one)
            else:
                beside = beside + (below[k, v, part, :] + above[k, v, part, :])
            new = onsite[part, :] * here - inv_row * beside
            out = []
            if landed is None:
                new = new - basis[k, v, part, :]
                basis[k + 2, v, part, :] = new
                out.append(new * new)
            out.append(new * here)
            added = []
            for (h, l), x in zip(carry, out):
                h, e = two_sum(h, fold(x))
                added.append((h, l + e))
            return tuple(added)

        return lax.fori_loop(0, count // block_rows, block, totals)

    sub = lax.broadcasted_iota(jnp.int32, (8, 128), 0)
    lane = lax.broadcasted_iota(jnp.int32, (8, 128), 1)

    def around(h, l, shift_by, ways, axis):
        turned = [(h, l)] + [
            (pltpu.roll(h, i * shift_by, axis), pltpu.roll(l, i * shift_by, axis))
            for i in range(1, ways)
        ]
        total, lost = tree_rows([a for a, _ in turned])
        lows = [b for _, b in turned]
        while len(lows) > 1:
            lows = [a + b for a, b in zip(lows[::2], lows[1::2])]
        return total, lows[0] + lost

    def lane_sums(items):
        high = jnp.zeros((8, 128), jnp.float32)
        low = jnp.zeros((8, 128), jnp.float32)
        target = jnp.full((8, 128), 1000, jnp.int32)
        for q, (h, l, place) in enumerate(items):
            for shift_by, ways in ((2, 4), (1, 2)):
                h, l = around(h, l, shift_by, ways, 0)
            high = jnp.where(sub == q, h, high)
            low = jnp.where(sub == q, l, low)
            target = jnp.where(sub == q, place, target)
        for shift_by, ways in ((32, 4), (8, 4), (2, 4), (1, 2)):
            high, low = around(high, low, shift_by, ways, 1)
        return jnp.where(lane == target, high, 0.0) + jnp.where(
            lane == target + 16, low, 0.0
        )

    def step(k, final_sends=False):
        for v in range(2):
            totals = (none, none)
            for c in range(CHUNKS):
                halo(k, v, c, True).wait_recv()
                halo(k, v, c, False).wait_recv()
                totals = sweep(k, v, c * rows, rows, totals)
                halo(k + 1, v, c, True, final_sends).start()
                halo(k + 1, v, c, False, final_sends).start()
            for q in range(2):
                stats[4 * k + 2 * v + q, 0], stats[4 * k + 2 * v + q, 1] = squeeze(totals[q])

    def last_step():
        k = STEPS - 1
        ends = []
        for v in range(2):
            totals = (none,)
            for c in range(CHUNKS):
                if v == 1 and c == CHUNKS - 1:
                    places = [64 * (i % 4 // 2) + (8 + i // 4 if i % 2 else 1 + i // 4) for i in range(4 * k)]
                    places += [0, 64]
                    packed = jnp.zeros((8, 128), jnp.float32)
                    for i in range(0, len(places), 8):
                        packed = packed + lane_sums(
                            [(stats[j, 0], stats[j, 1], places[j]) for j in range(i, min(i + 8, len(places)))]
                        )
                halo(k, v, c, True, True).wait_recv()
                halo(k, v, c, False, True).wait_recv()
                totals = sweep(k, v, c * rows, rows // 2, totals, below)
                totals = sweep(k, v, c * rows + rows // 2, rows // 2, totals, above)
            ends.append(squeeze(totals[0]))
        return packed + lane_sums([(h, l, 64 * v + 8 + k) for v, (h, l) in enumerate(ends)])

    say(1, 1)
    step(0)

    def middle(k, distance):
        @pl.when(k <= rounds)
        def _():
            hear(k)

        @pl.when(k < rounds)
        def _():
            say(k + 1, distance)

        step(k)
        return distance * 2

    lax.fori_loop(1, STEPS - 2, middle, 2)
    for k in (STEPS - 2, STEPS - 1):
        if k <= rounds:
            hear(k)
        if k < rounds:
            say(k + 1, 2**k)
        if k == STEPS - 2:
            step(k, final_sends=True)
    packed = last_step()
    if rounds == STEPS:
        hear(rounds)

    for shift_by in (4, 2, 1):
        packed = packed + pltpu.roll(packed, shift_by, 0)

    row_lane = lax.broadcasted_iota(jnp.int32, (1, 128), 1)
    is_high = lax.rem(row_lane, 64) < 16

    def drain(k, _):
        for v in range(2):
            for c in range(CHUNKS):
                halo(k, v, c, True).wait_send()
                halo(k, v, c, False).wait_send()
        return None

    def drain_all():
        lax.fori_loop(0, STEPS - 1, drain, None)
        for v in range(2):
            for c in range(CHUNKS):
                halo(STEPS - 1, v, c, True, True).wait_send()
                halo(STEPS - 1, v, c, False, True).wait_send()

    def exchange(row, staging, slots, place, peers, send, recv, meanwhile):
        def copy(i, slot):
            return pltpu.make_async_remote_copy(
                src_ref=staging,
                dst_ref=slots.at[slot],
                send_sem=send.at[i],
                recv_sem=recv.at[slot],
                device_id=(peers[i][1],),
                device_id_type=MESH,
            )

        staging[...] = row
        slots[place] = row
        for i in range(len(peers)):
            copy(i, place).start()
        meanwhile()
        for i in reversed(range(len(peers))):
            copy(i, peers[i][0]).wait_recv()
        total, lost = tree_rows([slots[i] for i in range(len(peers) + 1)])
        return jnp.where(is_high, total, total + pltpu.roll(lost, 16, 1)), [
            copy(i, place) for i in range(len(peers))
        ]

    row, sent = exchange(
        packed[0:1], row_b, far, team, far_peers, far_send, far_recv, drain_all
    )

    def drain_first():
        for copy in sent:
            copy.wait_send()

    row, more = exchange(
        row, row_a, near, mine, near_peers, near_send, near_recv, drain_first
    )
    row = jnp.where(row_lane == 40, shift, row)
    row = jnp.where(row_lane == 41, inv_row[:, :128], row)
    row_ref[...] = row
    for copy in more:
        copy.wait_send()


def combine(
    row_ref,
    basis,
    field_ref,
    diag_ref,
    off_ref,
    mom_ref,
    field,
    diag_out,
    off_out,
    mom_out,
    table,
    out_sem,
    small_sem,
):
    ny, nx = field.shape[1:]

    row = row_ref[...]
    row_lane = lax.broadcasted_iota(jnp.int32, (1, 128), 1)
    shift = jnp.sum(jnp.where(row_lane == 40, row, 0.0), axis=1, keepdims=True)
    inv_row = jnp.sum(jnp.where(row_lane == 41, row, 0.0), axis=1, keepdims=True)
    tall_row = lax.broadcasted_iota(jnp.int32, (32, 128), 0)
    tall_lane = lax.broadcasted_iota(jnp.int32, (32, 128), 1)
    spread_row = jnp.broadcast_to(row, (32, 128))
    first = jnp.sum(jnp.where(tall_lane == tall_row, spread_row, 0.0), axis=1, keepdims=True)
    second = jnp.sum(
        jnp.where(tall_lane == tall_row + 64, spread_row, 0.0), axis=1, keepdims=True
    )
    table[...] = jnp.where(tall_lane < 64, first, second)

    norms = [(table[k : k + 1, :], table[16 + k : 17 + k, :]) for k in range(STEPS)]
    crosses = [(table[8 + k : 9 + k, :], table[24 + k : 25 + k, :]) for k in range(STEPS)]
    diag, square = coefficients(norms, crosses)

    width = jnp.broadcast_to(1.0 / inv_row, (1, 128))
    alphas = [shift + width * a[0] for a in diag]
    betas = [width * jnp.sqrt(b[0]) for b in square]
    zero = jnp.zeros((1, 128), jnp.float32)
    left = [zero] + betas
    right = betas + [zero]
    emin = functools.reduce(jnp.minimum, [a - p - q for a, p, q in zip(alphas, left, right)])
    emax = functools.reduce(jnp.maximum, [a + p + q for a, p, q in zip(alphas, left, right)])
    center = (emax + emin) * 0.5
    inv_half = 1.0 / (0.55 * (emax - emin))
    slope = width * inv_half
    offset = (shift - center) * inv_half

    def apply(poly):
        around = [zero] + poly + [zero]
        out = []
        for k in range(len(poly) + 1):
            value = slope * around[k] if k else None
            if k < len(poly):
                value = offset * poly[k] if value is None else value + offset * poly[k]
            if k + 2 < len(around) - 1:
                value = value + slope * around[k + 2]
            out.append(value)
        return out

    t0 = [zero + 1.0]
    t1 = apply(t0)
    t2 = [2.0 * q for q in apply(t1)]
    t2[0] = t2[0] - 1.0
    t3 = [2.0 * q for q in apply(t2)]
    t3 = [q - t1[k] if k < 2 else q for k, q in enumerate(t3)]

    inv_norm = 1.0 / norms[0][0]
    size = [q[0] * inv_norm for q in norms[:4]]
    cross = [q[0] * inv_norm for q in crosses[:3]]
    skip = pair_sub(norms[1], norms[0])[0] * inv_norm
    skip_next = pair_sub(norms[2], norms[0])[0] * inv_norm
    skip_two = pair_sub(crosses[1], crosses[0])[0] * inv_norm
    gram = [
        [zero + 1.0, cross[0], skip, skip_two],
        [cross[0], size[1], cross[1], skip_next],
        [skip, cross[1], size[2], cross[2]],
        [skip_two, skip_next, cross[2], size[3]],
    ]

    def inner(p, q):
        return sum(
            a * sum(b * gram[i][j] for j, b in enumerate(q)) for i, a in enumerate(p)
        )

    d01 = inner(t0, t1)
    moments = [
        d01,
        inner(t0, t2),
        inner(t0, t3),
        2.0 * inner(t2, t2) - 1.0,
        2.0 * inner(t3, t2) - d01,
        2.0 * inner(t3, t3) - 1.0,
    ]

    def emit(ref, values):
        packed = zero
        for k, value in enumerate(values):
            packed = jnp.where(lax.rem(row_lane, 64) == k, value, packed)
        ref[0:1, :] = packed[:, : len(values)]
        ref[1:2, :] = pltpu.roll(packed, 64, 1)[:, : len(values)]

    small = []
    for k, (stage, ref, values) in enumerate(
        [(diag_out, diag_ref, alphas), (off_out, off_ref, betas), (mom_out, mom_ref, moments)]
    ):
        emit(stage, values)
        small.append(pltpu.make_async_copy(stage, ref, small_sem.at[k]))

    half = ny // 4

    def store(v, i):
        part = pl.ds(i * half, half)
        return pltpu.make_async_copy(
            field.at[v, part], field_ref.at[v, 0, part], out_sem.at[v, i]
        )

    for v in range(2):
        own = row_lane < 64 if v == 0 else row_lane >= 64
        scale = [jnp.where(own, q, pltpu.roll(q, 64, 1)) for q in t3]
        scale = [jnp.concatenate([q, q], axis=1) for q in scale]
        for i in range(4):

            def finish(b, _):
                part = pl.ds(pl.multiple_of(i * half + b * BLOCK, BLOCK), BLOCK)
                value = scale[0] * basis[1, v, part, :] + scale[1] * basis[2, v, part, :]
                value = value + scale[2] * basis[3, v, part, :]
                field[v, part, :] = value + scale[3] * basis[4, v, part, :]
                return None

            lax.fori_loop(0, half // BLOCK, finish, None)
            store(v, i).start()
        if v == 0:
            for copy in small:
                copy.start()

    for v in range(2):
        for i in range(4):
            store(v, i).wait()
    for copy in small:
        copy.wait()


def solution(mesh):
    n = mesh.shape["slab"]
    group = 16 if n >= 128 else 4

    def shards(start_vectors, levels, energies):
        vecs, _, ny, nx = start_vectors.shape
        f32 = jnp.float32
        dma = pltpu.SemaphoreType.DMA
        vmem = pl.BlockSpec(memory_space=pltpu.VMEM)
        hbm = pl.BlockSpec(memory_space=pltpu.HBM)
        halo_sem = dma((STEPS, vecs, CHUNKS))
        groups = n // group
        row, basis = pl.pallas_call(
            functools.partial(iterate, n, group),
            out_shape=(
                pltpu.VMEM((1, 128), f32),
                pltpu.VMEM((STEPS + 1, vecs, ny, nx), f32),
            ),
            in_specs=[hbm, hbm, hbm],
            out_specs=(vmem, vmem),
            scratch_shapes=[
                pltpu.VMEM((STEPS, vecs, ny, nx), f32),
                pltpu.VMEM((STEPS, vecs, ny, nx), f32),
                pltpu.VMEM((ny, nx), f32),
                pltpu.VMEM((ny, nx), jnp.int32),
                pltpu.VMEM((4 * STEPS - 2, 2, 8, 128), f32),
                pltpu.VMEM((1, 128), f32),
                pltpu.VMEM((1, 128), f32),
                pltpu.VMEM((group, 1, 128), f32),
                pltpu.VMEM((groups, 1, 128), f32),
                dma((2 * CHUNKS + 2,)),
                pltpu.SMEM(energies.shape, f32),
                pltpu.SemaphoreType.REGULAR((STEPS,)),
                halo_sem,
                halo_sem,
                halo_sem,
                halo_sem,
                dma((group,)),
                dma((group,)),
                dma((groups,)),
                dma((groups,)),
            ],
            compiler_params=pltpu.CompilerParams(
                collective_id=0, has_side_effects=True, vmem_limit_bytes=62_000_000
            ),
        )(start_vectors, levels, energies)
        return pl.pallas_call(
            combine,
            out_shape=(
                jax.ShapeDtypeStruct(start_vectors.shape, f32),
                jax.ShapeDtypeStruct((vecs, STEPS), f32),
                jax.ShapeDtypeStruct((vecs, STEPS - 1), f32),
                jax.ShapeDtypeStruct((vecs, 6), f32),
            ),
            in_specs=[vmem, vmem],
            out_specs=(hbm, hbm, hbm, hbm),
            scratch_shapes=[
                pltpu.VMEM((vecs, ny, nx), f32),
                pltpu.VMEM((vecs, STEPS), f32),
                pltpu.VMEM((vecs, STEPS - 1), f32),
                pltpu.VMEM((vecs, 6), f32),
                pltpu.VMEM((32, 128), f32),
                dma((vecs, 4)),
                dma((3,)),
            ],
            compiler_params=pltpu.CompilerParams(vmem_limit_bytes=8 * 2**20),
        )(row, basis)

    return jax.shard_map(
        shards,
        mesh=mesh,
        in_specs=(P(None, "slab", None, None), P("slab", None, None), P()),
        out_specs=(P(None, "slab", None, None), P(), P(), P()),
        check_vma=False,
    )
```

```python
import functools

import jax
import jax.numpy as jnp
from jax import lax
from jax.experimental import pallas as pl
from jax.experimental.pallas import tpu as pltpu
from jax.sharding import PartitionSpec as P

STEPS = 8
CHUNKS = 4
BLOCK = 32
MESH = pl.DeviceIdType.MESH


def two_sum(a, b):
    s = a + b
    t = s - a
    return s, (a - (s - t)) + (b - t)


def fast_two_sum(a, b):
    s = a + b
    return s, b - (s - a)


def split(a):
    t = a * 4097.0
    high = t - (t - a)
    return high, a - high


def two_prod(a, b):
    p = a * b
    ah, al = split(a)
    bh, bl = split(b)
    return p, ((ah * bh - p) + ah * bl + al * bh) + al * bl


def pair_add(a, b):
    s, e = two_sum(a[0], b[0])
    return fast_two_sum(s, e + (a[1] + b[1]))


def pair_neg(a):
    return -a[0], -a[1]


def pair_sub(a, b):
    return pair_add(a, pair_neg(b))


def pair_mul(a, b):
    p, e = two_prod(a[0], b[0])
    return fast_two_sum(p, e + (a[0] * b[1] + a[1] * b[0]))


def pair_div(a, b):
    inv = 1.0 / b[0]
    first = a[0] * inv
    p, e = two_prod(first, b[0])
    rest = (a[0] - p) - e + a[1] - first * b[1]
    return fast_two_sum(first, rest * inv)


def tree_rows(rows):
    lost = None
    while len(rows) > 1:
        sums = []
        for a, b in zip(rows[::2], rows[1::2]):
            s, e = two_sum(a, b)
            sums.append(s)
            lost = e if lost is None else lost + e
        rows = sums
    return rows[0], lost


def coefficients(norms, crosses):
    nu = []
    for k in range(STEPS):
        if k == 0:
            nu += [norms[0], crosses[0]]
        elif k < STEPS - 1:
            nu += [pair_sub(norms[k], norms[k - 1]), pair_sub(crosses[k], crosses[k - 1])]
        else:
            twice = pair_add(crosses[k - 1], crosses[k - 1])
            nu += [pair_sub(norms[k], norms[k - 1]), pair_sub(crosses[k], twice)]
    older, old = {}, dict(enumerate(nu))
    ratio = pair_div(old[1], old[0])
    diag, square = [ratio], []
    for k in range(1, STEPS):
        new = {}
        for l in range(k, 2 * STEPS - k):
            p, e = two_prod(diag[-1][0], old[l][0])
            e = e + (diag[-1][0] * old[l][1] + diag[-1][1] * old[l][0])
            sides, lost = two_sum(old[l + 1][0], old[l - 1][0])
            lost = lost + (old[l + 1][1] + old[l - 1][1])
            term, d = two_sum(sides, -p)
            lost = (lost - e) + d
            if k > 1:
                p, e = two_prod(square[-1][0], older[l][0])
                e = e + (square[-1][0] * older[l][1] + square[-1][1] * older[l][0])
                term, d = two_sum(term, -p)
                lost = (lost - e) + d
            term = fast_two_sum(term, lost)
            new[l] = term
        square.append(pair_div(new[k], old[k - 1]))
        next_ratio = pair_div(new[k + 1], new[k])
        diag.append(pair_sub(next_ratio, ratio))
        ratio = next_ratio
        older, old = old, new
    return diag, square


def scaling(en_ref):
    energies = [en_ref[i] for i in range(en_ref.shape[0])]
    shift = sum(energies[1:], energies[0]) * (1.0 / len(energies))
    spread = sum((e - shift) * (e - shift) for e in energies) * (1.0 / len(energies))
    return energies, shift, spread + 9.0


def inverse_width(square, nx):
    return 1.0 / jnp.sqrt(jnp.full((1, nx), square, jnp.float32))


def iterate(
    n,
    group,
    sv_ref,
    lev_ref,
    en_ref,
    row_ref,
    basis,
    below,
    above,
    onsite,
    levels,
    stats,
    row_a,
    row_b,
    near,
    far,
    load_sem,
    en_smem,
    met,
    up_send,
    up_recv,
    down_send,
    down_recv,
    near_send,
    near_recv,
    far_send,
    far_recv,
):
    ny, nx = onsite.shape
    rows = ny // CHUNKS
    block_rows = min(BLOCK, rows // 2)
    groups = n // group
    me = lax.axis_index("slab")
    up = lax.rem(me + 1, n)
    down = lax.rem(me + n - 1, n)
    mine = lax.rem(me, group)
    team = me // group

    def ring(d, size):
        return min(d, size - d)

    near_peers = []
    for d in sorted(range(1, group), key=lambda d: -ring(d, group)):
        place = lax.rem(mine + d, group)
        near_peers.append((place, team * group + place))
    long = min(8, groups)
    wide = groups // long
    far_peers = []
    steps = [(a, b) for a in range(wide) for b in range(long) if (a, b) != (0, 0)]
    for a, b in sorted(steps, key=lambda ab: -ring(ab[0], wide) - ring(ab[1], long)):
        place = lax.rem(team // long + a, wide) * long + lax.rem(team + b, long)
        far_peers.append((place, place * group + mine))

    def tell(sem, device):
        pl.semaphore_signal(sem, inc=1, device_id=(device,), device_id_type=MESH)

    barrier = pltpu.get_barrier_semaphore()
    tell(barrier, up)
    tell(barrier, down)

    def load(v, c):
        part = pl.ds(c * rows, rows)
        return pltpu.make_async_copy(
            sv_ref.at[v, 0, part], basis.at[1, v, part], load_sem.at[v * CHUNKS + c]
        )

    load_levels = pltpu.make_async_copy(lev_ref.at[0], levels, load_sem.at[2 * CHUNKS])
    for v in range(2):
        for c in range(CHUNKS):
            load(v, c).start()
    load_levels.start()
    load_energies = pltpu.make_async_copy(en_ref, en_smem, load_sem.at[2 * CHUNKS + 1])
    load_energies.start()

    pl.semaphore_wait(barrier, 2)

    rounds = n.bit_length() - 2

    def hear(r):
        pl.semaphore_wait(met.at[r - 1], 2)

    def say(r, distance):
        tell(met.at[r - 1], lax.rem(me + distance, n))
        tell(met.at[r - 1], lax.rem(me + n - distance, n))

    def halo(k, v, c, upward, half=False):
        part = pl.ds(c * rows, rows)
        if half:
            part = pl.ds(c * rows + (0 if upward else rows // 2), rows // 2)
        landing, send, recv, device = (
            (below, up_send, up_recv, up) if upward else (above, down_send, down_recv, down)
        )
        return pltpu.make_async_remote_copy(
            src_ref=basis.at[k + 1, v, part],
            dst_ref=landing.at[k, v, part],
            send_sem=send.at[k, v, c],
            recv_sem=recv.at[k, v, c],
            device_id=(device,),
            device_id_type=MESH,
        )

    for v in range(2):
        for c in range(CHUNKS):
            load(v, c).wait()
            halo(0, v, c, True).start()
            halo(0, v, c, False).start()

    load_energies.wait()
    energies, shift, square = scaling(en_smem)
    inv_row = inverse_width(square, nx)

    load_levels.wait()

    def fold(x):
        parts = [x[i : i + 8] for i in range(0, x.shape[0], 8)]
        while len(parts) > 1:
            parts = [a + b for a, b in zip(parts[::2], parts[1::2])]
        return parts[0]

    def place_onsite(b, carry):
        part = pl.ds(pl.multiple_of(b * block_rows, block_rows), block_rows)
        ids = levels[part, :]
        value = jnp.full((block_rows, nx), energies[0], jnp.float32)
        for i in range(1, len(energies)):
            value = jnp.where(ids == i, energies[i], value)
        onsite[part, :] = (value - shift) * inv_row
        out = []
        for v in range(2):
            basis[0, v, part, :] = jnp.zeros((block_rows, nx), jnp.float32)
            here = basis[1, v, part, :]
            h, e = two_sum(carry[v][0], fold(here * here))
            out.append((h, carry[v][1] + e))
        return tuple(out)

    def squeeze(total):
        h, l = total
        h, e = two_sum(h[:, :128], h[:, 128:])
        return h, (l[:, :128] + l[:, 128:]) + e

    zero_rows = jnp.zeros((8, nx), jnp.float32)
    none = (zero_rows, zero_rows)
    first_norms = lax.fori_loop(0, ny // block_rows, place_onsite, (none, none))
    for v in range(2):
        stats[4 * STEPS - 4 + v, 0], stats[4 * STEPS - 4 + v, 1] = squeeze(first_norms[v])

    def sweep(k, v, first, count, totals, landed=None):
        def block(b, carry):
            start = pl.multiple_of(first + b * block_rows, block_rows)
            part = pl.ds(start, block_rows)
            before = pl.ds(pl.multiple_of(lax.rem(start + (ny - 8), ny), 8), 8)
            after = pl.ds(pl.multiple_of(lax.rem(start + block_rows, ny), 8), 8)
            here = basis[k + 1, v, part, :]
            tall = jnp.concatenate(
                [basis[k + 1, v, before, :], here, basis[k + 1, v, after, :]], axis=0
            )
            height = block_rows + 16
            beside = pltpu.roll(tall, 1, 0)[8 : 8 + block_rows]
            beside = beside + pltpu.roll(tall, height - 1, 0)[8 : 8 + block_rows]
            beside = beside + (pltpu.roll(here, 1, 1) + pltpu.roll(here, nx - 1, 1))
            if landed is not None:
                one = landed[k, v, part, :]
                beside = beside + (one + one)
            else:
                beside = beside + (below[k, v, part, :] + above[k, v, part, :])
            new = onsite[part, :] * here - inv_row * beside
            out = []
            if landed is None:
                new = new - basis[k, v, part, :]
                basis[k + 2, v, part, :] = new
                out.append(new * new)
            out.append(new * here)
            added = []
            for (h, l), x in zip(carry, out):
                h, e = two_sum(h, fold(x))
                added.append((h, l + e))
            return tuple(added)

        return lax.fori_loop(0, count // block_rows, block, totals, unroll=True)

    sub = lax.broadcasted_iota(jnp.int32, (8, 128), 0)
    lane = lax.broadcasted_iota(jnp.int32, (8, 128), 1)

    def around(h, l, shift_by, ways, axis):
        turned = [(h, l)] + [
            (pltpu.roll(h, i * shift_by, axis), pltpu.roll(l, i * shift_by, axis))
            for i in range(1, ways)
        ]
        total, lost = tree_rows([a for a, _ in turned])
        lows = [b for _, b in turned]
        while len(lows) > 1:
            lows = [a + b for a, b in zip(lows[::2], lows[1::2])]
        return total, lows[0] + lost

    def lane_sums(items):
        high = jnp.zeros((8, 128), jnp.float32)
        low = jnp.zeros((8, 128), jnp.float32)
        target = jnp.full((8, 128), 1000, jnp.int32)
        for q, (h, l, place) in enumerate(items):
            for shift_by, ways in ((2, 4), (1, 2)):
                h, l = around(h, l, shift_by, ways, 0)
            high = jnp.where(sub == q, h, high)
            low = jnp.where(sub == q, l, low)
            target = jnp.where(sub == q, place, target)
        for shift_by, ways in ((32, 4), (8, 4), (2, 4), (1, 2)):
            high, low = around(high, low, shift_by, ways, 1)
        return jnp.where(lane == target, high, 0.0) + jnp.where(
            lane == target + 16, low, 0.0
        )

    def step(k, final_sends=False):
        for v in range(2):
            totals = (none, none)
            for c in range(CHUNKS):
                halo(k, v, c, True).wait_recv()
                halo(k, v, c, False).wait_recv()
                totals = sweep(k, v, c * rows, rows, totals)
                halo(k + 1, v, c, True, final_sends).start()
                halo(k + 1, v, c, False, final_sends).start()
            for q in range(2):
                stats[4 * k + 2 * v + q, 0], stats[4 * k + 2 * v + q, 1] = squeeze(totals[q])

    def last_step():
        k = STEPS - 1
        ends = []
        for v in range(2):
            totals = (none,)
            for c in range(CHUNKS):
                if v == 1 and c == CHUNKS - 1:
                    places = [64 * (i % 4 // 2) + (8 + i // 4 if i % 2 else 1 + i // 4) for i in range(4 * k)]
                    places += [0, 64]
                    packed = jnp.zeros((8, 128), jnp.float32)
                    for i in range(0, len(places), 8):
                        packed = packed + lane_sums(
                            [(stats[j, 0], stats[j, 1], places[j]) for j in range(i, min(i + 8, len(places)))]
                        )
                halo(k, v, c, True, True).wait_recv()
                halo(k, v, c, False, True).wait_recv()
                totals = sweep(k, v, c * rows, rows // 2, totals, below)
                totals = sweep(k, v, c * rows + rows // 2, rows // 2, totals, above)
            ends.append(squeeze(totals[0]))
        return packed + lane_sums([(h, l, 64 * v + 8 + k) for v, (h, l) in enumerate(ends)])

    say(1, 1)
    step(0)

    def middle(k, distance):
        @pl.when(k <= rounds)
        def _():
            hear(k)

        @pl.when(k < rounds)
        def _():
            say(k + 1, distance)

        step(k)
        return distance * 2

    lax.fori_loop(1, STEPS - 2, middle, 2)
    for k in (STEPS - 2, STEPS - 1):
        if k <= rounds:
            hear(k)
        if k < rounds:
            say(k + 1, 2**k)
        if k == STEPS - 2:
            step(k, final_sends=True)
    packed = last_step()
    if rounds == STEPS:
        hear(rounds)

    for shift_by in (4, 2, 1):
        packed = packed + pltpu.roll(packed, shift_by, 0)

    row_lane = lax.broadcasted_iota(jnp.int32, (1, 128), 1)
    is_high = lax.rem(row_lane, 64) < 16

    def drain(k, _):
        for v in range(2):
            for c in range(CHUNKS):
                halo(k, v, c, True).wait_send()
                halo(k, v, c, False).wait_send()
        return None

    def drain_all():
        lax.fori_loop(0, STEPS - 1, drain, None)
        for v in range(2):
            for c in range(CHUNKS):
                halo(STEPS - 1, v, c, True, True).wait_send()
                halo(STEPS - 1, v, c, False, True).wait_send()

    def exchange(row, staging, slots, place, peers, send, recv, meanwhile):
        def copy(i, slot):
            return pltpu.make_async_remote_copy(
                src_ref=staging,
                dst_ref=slots.at[slot],
                send_sem=send.at[i],
                recv_sem=recv.at[slot],
                device_id=(peers[i][1],),
                device_id_type=MESH,
            )

        staging[...] = row
        slots[place] = row
        for i in range(len(peers)):
            copy(i, place).start()
        meanwhile()
        for i in reversed(range(len(peers))):
            copy(i, peers[i][0]).wait_recv()
        total, lost = tree_rows([slots[i] for i in range(len(peers) + 1)])
        return jnp.where(is_high, total, total + pltpu.roll(lost, 16, 1)), [
            copy(i, place) for i in range(len(peers))
        ]

    row, sent = exchange(
        packed[0:1], row_b, far, team, far_peers, far_send, far_recv, drain_all
    )

    def drain_first():
        for copy in sent:
            copy.wait_send()

    row, more = exchange(
        row, row_a, near, mine, near_peers, near_send, near_recv, drain_first
    )
    row = jnp.where(row_lane == 40, shift, row)
    row = jnp.where(row_lane == 41, inv_row[:, :128], row)
    row_ref[...] = row
    for copy in more:
        copy.wait_send()


def combine(
    row_ref,
    basis,
    field_ref,
    diag_ref,
    off_ref,
    mom_ref,
    field,
    diag_out,
    off_out,
    mom_out,
    table,
    out_sem,
    small_sem,
):
    ny, nx = field.shape[1:]

    row = row_ref[...]
    row_lane = lax.broadcasted_iota(jnp.int32, (1, 128), 1)
    shift = jnp.sum(jnp.where(row_lane == 40, row, 0.0), axis=1, keepdims=True)
    inv_row = jnp.sum(jnp.where(row_lane == 41, row, 0.0), axis=1, keepdims=True)
    tall_row = lax.broadcasted_iota(jnp.int32, (32, 128), 0)
    tall_lane = lax.broadcasted_iota(jnp.int32, (32, 128), 1)
    spread_row = jnp.broadcast_to(row, (32, 128))
    first = jnp.sum(jnp.where(tall_lane == tall_row, spread_row, 0.0), axis=1, keepdims=True)
    second = jnp.sum(
        jnp.where(tall_lane == tall_row + 64, spread_row, 0.0), axis=1, keepdims=True
    )
    table[...] = jnp.where(tall_lane < 64, first, second)

    norms = [(table[k : k + 1, :], table[16 + k : 17 + k, :]) for k in range(STEPS)]
    crosses = [(table[8 + k : 9 + k, :], table[24 + k : 25 + k, :]) for k in range(STEPS)]
    diag, square = coefficients(norms, crosses)

    width = jnp.broadcast_to(1.0 / inv_row, (1, 128))
    alphas = [shift + width * a[0] for a in diag]
    betas = [width * jnp.sqrt(b[0]) for b in square]
    zero = jnp.zeros((1, 128), jnp.float32)
    left = [zero] + betas
    right = betas + [zero]
    emin = functools.reduce(jnp.minimum, [a - p - q for a, p, q in zip(alphas, left, right)])
    emax = functools.reduce(jnp.maximum, [a + p + q for a, p, q in zip(alphas, left, right)])
    center = (emax + emin) * 0.5
    inv_half = 1.0 / (0.55 * (emax - emin))
    slope = width * inv_half
    offset = (shift - center) * inv_half

    def apply(poly):
        around = [zero] + poly + [zero]
        out = []
        for k in range(len(poly) + 1):
            value = slope * around[k] if k else None
            if k < len(poly):
                value = offset * poly[k] if value is None else value + offset * poly[k]
            if k + 2 < len(around) - 1:
                value = value + slope * around[k + 2]
            out.append(value)
        return out

    t0 = [zero + 1.0]
    t1 = apply(t0)
    t2 = [2.0 * q for q in apply(t1)]
    t2[0] = t2[0] - 1.0
    t3 = [2.0 * q for q in apply(t2)]
    t3 = [q - t1[k] if k < 2 else q for k, q in enumerate(t3)]

    inv_norm = 1.0 / norms[0][0]
    size = [q[0] * inv_norm for q in norms[:4]]
    cross = [q[0] * inv_norm for q in crosses[:3]]
    skip = pair_sub(norms[1], norms[0])[0] * inv_norm
    skip_next = pair_sub(norms[2], norms[0])[0] * inv_norm
    skip_two = pair_sub(crosses[1], crosses[0])[0] * inv_norm
    gram = [
        [zero + 1.0, cross[0], skip, skip_two],
        [cross[0], size[1], cross[1], skip_next],
        [skip, cross[1], size[2], cross[2]],
        [skip_two, skip_next, cross[2], size[3]],
    ]

    def inner(p, q):
        return sum(
            a * sum(b * gram[i][j] for j, b in enumerate(q)) for i, a in enumerate(p)
        )

    d01 = inner(t0, t1)
    moments = [
        d01,
        inner(t0, t2),
        inner(t0, t3),
        2.0 * inner(t2, t2) - 1.0,
        2.0 * inner(t3, t2) - d01,
        2.0 * inner(t3, t3) - 1.0,
    ]

    def emit(ref, values):
        packed = zero
        for k, value in enumerate(values):
            packed = jnp.where(lax.rem(row_lane, 64) == k, value, packed)
        ref[0:1, :] = packed[:, : len(values)]
        ref[1:2, :] = pltpu.roll(packed, 64, 1)[:, : len(values)]

    small = []
    for k, (stage, ref, values) in enumerate(
        [(diag_out, diag_ref, alphas), (off_out, off_ref, betas), (mom_out, mom_ref, moments)]
    ):
        emit(stage, values)
        small.append(pltpu.make_async_copy(stage, ref, small_sem.at[k]))

    half = ny // 4

    def store(v, i):
        part = pl.ds(i * half, half)
        return pltpu.make_async_copy(
            field.at[v, part], field_ref.at[v, 0, part], out_sem.at[v, i]
        )

    for v in range(2):
        own = row_lane < 64 if v == 0 else row_lane >= 64
        scale = [jnp.where(own, q, pltpu.roll(q, 64, 1)) for q in t3]
        scale = [jnp.concatenate([q, q], axis=1) for q in scale]
        for i in range(4):

            def finish(b, _):
                part = pl.ds(pl.multiple_of(i * half + b * BLOCK, BLOCK), BLOCK)
                value = scale[0] * basis[1, v, part, :] + scale[1] * basis[2, v, part, :]
                value = value + scale[2] * basis[3, v, part, :]
                field[v, part, :] = value + scale[3] * basis[4, v, part, :]
                return None

            lax.fori_loop(0, half // BLOCK, finish, None, unroll=True)
            store(v, i).start()
        if v == 0:
            for copy in small:
                copy.start()

    for v in range(2):
        for i in range(4):
            store(v, i).wait()
    for copy in small:
        copy.wait()


def solution(mesh):
    n = mesh.shape["slab"]
    group = 16 if n >= 128 else 4

    def shards(start_vectors, levels, energies):
        vecs, _, ny, nx = start_vectors.shape
        f32 = jnp.float32
        dma = pltpu.SemaphoreType.DMA
        vmem = pl.BlockSpec(memory_space=pltpu.VMEM)
        hbm = pl.BlockSpec(memory_space=pltpu.HBM)
        halo_sem = dma((STEPS, vecs, CHUNKS))
        groups = n // group
        row, basis = pl.pallas_call(
            functools.partial(iterate, n, group),
            out_shape=(
                pltpu.VMEM((1, 128), f32),
                pltpu.VMEM((STEPS + 1, vecs, ny, nx), f32),
            ),
            in_specs=[hbm, hbm, hbm],
            out_specs=(vmem, vmem),
            scratch_shapes=[
                pltpu.VMEM((STEPS, vecs, ny, nx), f32),
                pltpu.VMEM((STEPS, vecs, ny, nx), f32),
                pltpu.VMEM((ny, nx), f32),
                pltpu.VMEM((ny, nx), jnp.int32),
                pltpu.VMEM((4 * STEPS - 2, 2, 8, 128), f32),
                pltpu.VMEM((1, 128), f32),
                pltpu.VMEM((1, 128), f32),
                pltpu.VMEM((group, 1, 128), f32),
                pltpu.VMEM((groups, 1, 128), f32),
                dma((2 * CHUNKS + 2,)),
                pltpu.SMEM(energies.shape, f32),
                pltpu.SemaphoreType.REGULAR((STEPS,)),
                halo_sem,
                halo_sem,
                halo_sem,
                halo_sem,
                dma((group,)),
                dma((group,)),
                dma((groups,)),
                dma((groups,)),
            ],
            compiler_params=pltpu.CompilerParams(
                collective_id=0, has_side_effects=True, vmem_limit_bytes=62_000_000
            ),
        )(start_vectors, levels, energies)
        return pl.pallas_call(
            combine,
            out_shape=(
                jax.ShapeDtypeStruct(start_vectors.shape, f32),
                jax.ShapeDtypeStruct((vecs, STEPS), f32),
                jax.ShapeDtypeStruct((vecs, STEPS - 1), f32),
                jax.ShapeDtypeStruct((vecs, 6), f32),
            ),
            in_specs=[vmem, vmem],
            out_specs=(hbm, hbm, hbm, hbm),
            scratch_shapes=[
                pltpu.VMEM((vecs, ny, nx), f32),
                pltpu.VMEM((vecs, STEPS), f32),
                pltpu.VMEM((vecs, STEPS - 1), f32),
                pltpu.VMEM((vecs, 6), f32),
                pltpu.VMEM((32, 128), f32),
                dma((vecs, 4)),
                dma((3,)),
            ],
            compiler_params=pltpu.CompilerParams(vmem_limit_bytes=8 * 2**20),
        )(row, basis)

    return jax.shard_map(
        shards,
        mesh=mesh,
        in_specs=(P(None, "slab", None, None), P("slab", None, None), P()),
        out_specs=(P(None, "slab", None, None), P(), P(), P()),
        check_vma=False,
    )
```
